32 devices in a mesh: dp: 2 (over y), tm: 4 (over z), rows: 4 (over x, core).
Axes of the slice: x: 2, y: 2, z: 4, core: 2. Of those that a mesh axis runs over, the one named last changes fastest.
Arguments:
- clips: bfloat16 [2, 8, 4, 128, 256], P('dp', 'tm', 'rows'), may hold values from -12 to 12
- weight: bfloat16 [3, 3, 3, 256, 256], replicated, may hold values from -0.078125 to 0.078125
- bias: float32 [256], replicated, may hold values from -1 to 1
- head: float32 [256], replicated, may hold values from -4 to 4
Outputs:
- grad_weight: float32 [3, 3, 3, 256, 256], replicated
- grad_bias: float32 [256], replicated
- grad_head: float32 [256], replicated
The draws below stay inside these ranges and needn't reach their ends.
All inputs are finite; a program needn't handle non-finite values.
Results may differ from the reference program's by a relative error of at most 0.0003.
Values may be sent and summed in bfloat16 or wider, within the bound.
A program may use at most 128 MiB of HBM per device.

```python
import jax
import jax.numpy as jnp
from jax import lax

C = 256
WID = 128
NT = 8
NH = 4
CLIPS = 2


def draw_clips(key, part):
    shape = (CLIPS, NT, NH, WID, C)
    frame_scale = 3.0 ** (jnp.arange(NT, dtype=jnp.float32) / max(NT - 1, 1))
    values = jnp.clip(jax.random.normal(key, shape, jnp.float32), -4.0, 4.0)
    return (values * frame_scale[None, :, None, None, None]).astype(jnp.bfloat16)


def centred(key, shape, width, most, kind=jnp.bfloat16):
    return jnp.clip(width * jax.random.normal(key, shape, jnp.float32), -most, most).astype(kind)


def setup_inputs(seed: int = 0) -> dict:
    seeds = jax.random.split(jax.random.key(seed), 5)
    return {
        "clips": draw_clips(jax.random.fold_in(seeds[4], 71), 0),
        "weight": centred(seeds[1], (3, 3, 3, C, C), (27 * C) ** -0.5, 0.078125),
        "bias": jnp.clip(jax.random.uniform(seeds[2], (C,), jnp.float32, -1.0, 1.0), -1.0, 1.0),
        "head": centred(seeds[3], (C,), 1.0, 4.0, jnp.float32),
    }


penalty_weight = 0.01


def conv_offsets(padded, weight, transpose):
    nclip, tpad, rpad, wpad, chans = padded.shape
    frames, rowsn, cols = tpad - 2, rpad - 2, wpad - 2
    total = jnp.zeros((nclip * frames * rowsn * cols, weight.shape[4]), jnp.float32)
    for a in range(3):
        for b in range(3):
            for d in range(3):
                if transpose:
                    piece = padded[:, 2 - a:2 - a + frames, 2 - b:2 - b + rowsn, 2 - d:2 - d + cols]
                    total = total + lax.dot_general(piece.reshape(-1, chans), weight[a, b, d], (((1,), (1,)), ((), ())), preferred_element_type=jnp.float32)
                else:
                    piece = padded[:, a:a + frames, b:b + rowsn, d:d + cols]
                    total = total + jnp.dot(piece.reshape(-1, chans), weight[a, b, d], preferred_element_type=jnp.float32)
    return total.reshape(nclip, frames, rowsn, cols, -1)


def correlate(padded, right):
    nclip, tpad, rpad, wpad, chans = padded.shape
    frames, rowsn, cols = tpad - 2, rpad - 2, wpad - 2
    right_rows = right.reshape(-1, right.shape[-1])
    blocks = []
    for a in range(3):
        for b in range(3):
            for d in range(3):
                piece = padded[:, a:a + frames, b:b + rowsn, d:d + cols].reshape(-1, chans)
                blocks.append(lax.dot_general(piece, right_rows, (((0,), (0,)), ((), ())), preferred_element_type=jnp.float32))
    return jnp.stack(blocks).reshape(3, 3, 3, chans, right.shape[-1])


def pad_all(field):
    return jnp.pad(field, ((0, 0), (1, 1), (1, 1), (1, 1), (0, 0)))


def reference(clips, weight, bias, head):
    clip_pad = pad_all(clips)
    pre = conv_offsets(clip_pad, weight, False) + bias
    sig = jax.nn.sigmoid(pre)
    slope = sig * (1.0 + pre * (1.0 - sig))
    curve = sig * (1.0 - sig) * (2.0 + pre * (1.0 - 2.0 * sig))
    score_grad = (head * slope).astype(jnp.bfloat16)
    input_grad = conv_offsets(pad_all(score_grad), weight, True).astype(jnp.bfloat16)
    grad_pad = pad_all(input_grad)
    back_grad = penalty_weight * conv_offsets(grad_pad, weight, False)
    pre_grad = back_grad * head * curve
    pre_grad_b = pre_grad.astype(jnp.bfloat16)
    grad_weight = penalty_weight * correlate(grad_pad, score_grad) + correlate(clip_pad, pre_grad_b)
    grad_bias = jnp.sum(pre_grad, axis=(0, 1, 2, 3))
    grad_head = jnp.sum(back_grad * slope, axis=(0, 1, 2, 3))
    return grad_weight, grad_bias, grad_head
```

```python
import functools
import math

import jax
import jax.numpy as jnp
from jax import lax
from jax.experimental import pallas as pl
from jax.experimental.pallas import tpu as pltpu
from jax.sharding import PartitionSpec as P

penalty_weight = 0.01
MESH = pl.DeviceIdType.MESH
SUB = 8
TAPS = 3
SPAN = 120.0
LANES = 128


def split_line(tm, most):
    line = 1
    while tm % (2 * line) == 0 and 2 * line <= most:
        line *= 2
    return line, tm // line


def decode(block, taps):
    unit = block[taps].astype(jnp.float32) * (1.0 / (SPAN * math.log(2.0)))
    return jnp.log(block[:taps].astype(jnp.float32)) * unit[None]


def encode(value):
    top = (jnp.max(jnp.abs(value), axis=0) * 1.01 + 1e-30).astype(jnp.bfloat16)
    rate = SPAN / top.astype(jnp.float32)
    return jnp.exp2(value * rate[None]).astype(jnp.bfloat16), top


def kernel(
    sizes, line, clips_ref, weight_ref, bias_ref, head_ref,
    out_ref, bias_out, head_out,
    w_ref, clip_pad, score_pad, grad_pad, acc, slope_ref, curve_ref,
    clip_all, grad_all, turned, slices, shifts, first, total, code, land, more, full,
    small_mine, small_plane, small_line,
    local_sem, halo_send, halo_recv, all_send, all_recv, pass_send, pass_recv,
    slice_send, slice_recv, part_send, part_recv, more_send, more_recv,
    line_send, line_recv, near_send, near_recv, turn_send, turn_recv, pair_send, pair_recv,
    sum_send, sum_recv, end_send, end_recv,
):
    dp, tm, rows = sizes
    frames, cols, chans = clips_ref.shape
    count = frames * cols
    plane = dp * rows
    share = chans // plane
    part = share // line
    taps = TAPS**2
    pair = 2 if rows % 2 == 0 else 1
    near = rows // pair
    me = {"dp": lax.axis_index("dp"), "tm": lax.axis_index("tm"), "rows": lax.axis_index("rows")}
    mine = me["dp"] * rows + me["rows"]

    def device(**moved):
        place = dict(me, **moved)
        return (place["dp"], place["tm"], place["rows"])

    def shift(axis, step):
        return lax.rem(me[axis] + step % dict(dp=dp, tm=tm, rows=rows)[axis], dict(dp=dp, tm=tm, rows=rows)[axis])

    def remote(src, dst, send, recv, target):
        return pltpu.make_async_remote_copy(
            src_ref=src, dst_ref=dst, send_sem=send, recv_sem=recv,
            device_id=target, device_id_type=MESH,
        )

    weight_copy = pltpu.make_async_copy(weight_ref, w_ref, local_sem.at[0])
    weight_copy.start()
    clip_copy = pltpu.make_async_copy(
        clips_ref, clip_pad.at[pl.ds(1, frames), 1], local_sem.at[1]
    )
    clip_copy.start()

    steps = {(i, t % tm, s) for i in range(dp) for t in (-1, 0, 1) for s in range(rows)}
    steps |= {(0, t, 0) for t in range(tm)}
    steps = sorted(steps - {(0, 0, 0)})
    barrier = pltpu.get_barrier_semaphore()
    for i, t, s in steps:
        pl.semaphore_signal(
            barrier, inc=1, device_id=(shift("dp", i), shift("tm", t), shift("rows", s)),
            device_id_type=MESH,
        )
    for axis, bound, fill in (
        ("rows", 0, lambda pad: pad.at[:, 0]), ("rows", rows - 1, lambda pad: pad.at[:, 2]),
        ("tm", 0, lambda pad: pad.at[0]), ("tm", tm - 1, lambda pad: pad.at[frames + 1]),
    ):
        @pl.when(me[axis] == bound)
        def _():
            for pad in (clip_pad, score_pad, grad_pad):
                at = fill(pad)
                at[...] = jnp.zeros(at.shape, at.dtype)
    for which in range(2):
        for edge in (0, rows + 1):
            shifts[which, :, edge] = jnp.zeros(shifts.shape[1:2] + shifts.shape[3:], shifts.dtype)
        for edge, bound in ((0, 0), (frames + 1, tm - 1)):
            @pl.when(me["tm"] == bound)
            def _():
                slices[which, :, edge] = jnp.zeros((plane, share, cols), slices.dtype)
    pl.semaphore_wait(barrier, len(steps))

    moves = [(t, r) for t in (-1, 0, 1) for r in (-1, 0, 1) if (t, r) != (0, 0)]

    def inside(t, r):
        ok = None
        for axis, step, size in (("tm", t, tm), ("rows", r, rows)):
            if step:
                cond = me[axis] > 0 if step < 0 else me[axis] < size - 1
                ok = cond if ok is None else jnp.logical_and(ok, cond)
        return ok

    def halo_copy(which, pad, source, t, r):
        slot = which * len(moves) + moves.index((t, r))
        if t == 0:
            here, there = pl.ds(0, frames), pl.ds(1, frames)
        elif t > 0:
            here, there = pl.ds(frames - 1, 1), pl.ds(0, 1)
        else:
            here, there = pl.ds(0, 1), pl.ds(frames + 1, 1)
        return pltpu.make_async_remote_copy(
            src_ref=source.at[here], dst_ref=pad.at[there, 1 - r],
            send_sem=halo_send.at[slot], recv_sem=halo_recv.at[slot],
            device_id=device(tm=me["tm"] + t, rows=me["rows"] + r), device_id_type=MESH,
        )

    def halo_start(which, pad, source):
        for t, r in moves:
            @pl.when(inside(t, r))
            def _():
                halo_copy(which, pad, source, t, r).start()

    def halo_wait(which, pad, source, level):
        for t, r in moves:
            if (t == 0) != level:
                continue

            @pl.when(inside(t, r))
            def _():
                halo_copy(which, pad, source, t, r).wait_send()

            @pl.when(inside(-t, -r))
            def _():
                halo_copy(which, pad, source, t, r).wait_recv()

    column = lax.rem(lax.broadcasted_iota(jnp.int32, (count, chans), 0), cols)

    def earlier(value):
        return jnp.where(column == 0, 0.0, pltpu.roll(value, 1, 0))

    def later(value):
        return jnp.where(column == cols - 1, 0.0, pltpu.roll(value, count - 1, 0))

    def conv(which, pad, source, transpose):
        def step(a):
            base = (TAPS - 1 - a) if transpose else a
            pieces = [
                pad[pl.ds(base, frames), (TAPS - 1 - b) if transpose else b].reshape(count, chans)
                for b in range(TAPS)
            ]
            left = jnp.concatenate(pieces, axis=1)
            for d in range(TAPS):
                taps = [w_ref[(a * TAPS + b) * TAPS + d] for b in range(TAPS)]
                if transpose:
                    part = lax.dot_general(
                        left, jnp.concatenate(taps, axis=1), (((1,), (1,)), ((), ())),
                        preferred_element_type=jnp.float32,
                    )
                else:
                    part = jnp.dot(
                        left, jnp.concatenate(taps, axis=0), preferred_element_type=jnp.float32
                    )
                acc[d] = part if a == 1 else acc[d] + part

        halo_wait(which, pad, source, True)
        step(1)
        halo_wait(which, pad, source, False)
        step(0)
        step(2)
        if transpose:
            return later(acc[0]) + acc[1] + earlier(acc[2])
        return earlier(acc[0]) + acc[1] + later(acc[2])


    close = [(i, s) for i in range(dp) for s in range(near) if (i, s) != (0, 0)]
    partner = me["rows"] + 1 - 2 * lax.rem(me["rows"], 2) if pair == 2 else me["rows"]

    def origin(i, s):
        return shift("dp", -i) * rows + shift("rows", -pair * s)

    def all_copy(which, buf, k):
        i, s = close[k]
        at = which * len(close) + k
        return remote(
            buf.at[mine], buf.at[mine], all_send.at[at], all_recv.at[at],
            device(dp=shift("dp", i), rows=shift("rows", pair * s)),
        )

    def pass_copy(which, buf, k):
        at = which * (len(close) + 1) + k
        block = buf.at[mine if k == len(close) else origin(*close[k])]
        return remote(block, block, pass_send.at[at], pass_recv.at[at], device(rows=partner))

    def all_start(which, buf):
        if pair == 2:
            pass_copy(which, buf, len(close)).start()
        for k in range(len(close)):
            all_copy(which, buf, k).start()

    def all_pass(which, buf):
        for k in range(len(close)):
            all_copy(which, buf, k).wait()
            if pair == 2:
                pass_copy(which, buf, k).start()

    def all_end(which, buf):
        if pair == 2:
            for k in range(len(close) + 1):
                pass_copy(which, buf, k).wait()

    def slice_copy(which, t, i, s):
        at = (which * 3 + t + 1) * plane + i * rows + s
        y, r = shift("dp", i), shift("rows", s)
        rest = pl.ds(pl.multiple_of((y * rows + r) * share, share), share)
        if t == 0:
            src, dst = turned.at[which, :, rest], slices.at[which, mine, pl.ds(1, frames)]
        elif t > 0:
            src, dst = turned.at[which, frames - 1, rest], slices.at[which, mine, 0]
        else:
            src, dst = turned.at[which, 0, rest], slices.at[which, mine, frames + 1]
        return remote(
            src, dst, slice_send.at[at], slice_recv.at[at],
            device(dp=y, rows=r, tm=me["tm"] + t),
        )

    pieces = [(i, s) for i in range(dp) for s in range(rows)]

    def slice_start(which, value):
        for f in range(frames):
            turned[which, f] = value[f * cols : (f + 1) * cols].T.astype(jnp.bfloat16)
        for t in (1, -1):
            @pl.when(inside(t, 0))
            def _():
                for i, s in pieces:
                    slice_copy(which, t, i, s).start()
        for i, s in pieces[1:]:
            slice_copy(which, 0, i, s).start()
        own = pl.ds(pl.multiple_of(mine * share, share), share)
        for f in range(frames):
            slices[which, mine, f + 1] = turned[which, f, own]

    lane = lax.broadcasted_iota(jnp.int32, (share, cols), 1)

    def slice_end(which):
        for t in (1, -1):
            @pl.when(inside(t, 0))
            def _():
                for i, s in pieces:
                    slice_copy(which, t, i, s).wait_send()

            @pl.when(inside(-t, 0))
            def _():
                for i, s in pieces:
                    slice_copy(which, t, i, s).wait_recv()
        for i, s in pieces[1:]:
            slice_copy(which, 0, i, s).wait()
        for j in range(plane):
            for f in range(frames + 2):
                value = slices[which, j, f].astype(jnp.float32)
                after = jnp.where(lane == cols - 1, 0.0, pltpu.roll(value, cols - 1, 1))
                before = jnp.where(lane == 0, 0.0, pltpu.roll(value, 1, 1))
                shifts[which, j // rows, j % rows + 1, f] = jnp.concatenate(
                    [after, value, before], axis=0
                ).astype(jnp.bfloat16)

    def correlate(which, buf, a):
        left = jnp.concatenate(
            [
                jnp.concatenate(
                    [
                        shifts[which, y, r + 2 - b, f + 2 - a]
                        for y in range(dp) for r in range(rows) for f in range(frames)
                    ],
                    axis=1,
                )
                for b in range(TAPS)
            ],
            axis=0,
        )
        right = buf[...].reshape(plane * count, chans)
        return jnp.dot(left, right, preferred_element_type=jnp.float32)

    halo_start(0, clip_pad, clips_ref)
    clip_copy.wait()
    clip_all[mine] = clip_pad[pl.ds(1, frames), 1].reshape(count, chans)
    all_start(0, clip_all)
    weight_copy.wait()
    pre = conv(0, clip_pad, clips_ref, False) + bias_ref[...]
    sig = jax.nn.sigmoid(pre)
    slope = sig * (1.0 + pre * (1.0 - sig))
    slope_ref[...] = slope
    curve_ref[...] = sig * (1.0 - sig) * (2.0 + pre * (1.0 - 2.0 * sig))
    score = (head_ref[...] * slope).astype(jnp.bfloat16)
    score_pad[pl.ds(1, frames), 1] = score.reshape(frames, cols, chans)
    score_own = score_pad.at[pl.ds(1, frames), 1]
    halo_start(1, score_pad, score_own)
    slice_start(0, score.astype(jnp.float32))
    all_pass(0, clip_all)

    input_grad = conv(1, score_pad, score_own, True).astype(jnp.bfloat16)
    grad_pad[pl.ds(1, frames), 1] = input_grad.reshape(frames, cols, chans)
    grad_own = grad_pad.at[pl.ds(1, frames), 1]
    halo_start(2, grad_pad, grad_own)
    grad_all[mine] = input_grad
    all_start(1, grad_all)
    slice_end(0)
    all_end(0, clip_all)

    back = penalty_weight * conv(2, grad_pad, grad_own, False)
    pre_grad = back * head_ref[...] * curve_ref[...]
    slice_start(1, pre_grad.astype(jnp.bfloat16).astype(jnp.float32))
    small_mine[...] = jnp.zeros_like(small_mine)
    small_mine[pl.ds(0, 1)] = jnp.sum(pre_grad, axis=0, keepdims=True)
    small_mine[pl.ds(1, 1)] = jnp.sum(back * slope_ref[...], axis=0, keepdims=True)

    def sum_copy(i, s):
        at = i * rows + s
        return remote(
            small_mine, small_plane.at[mine], sum_send.at[at], sum_recv.at[at],
            device(dp=shift("dp", i), rows=shift("rows", s)),
        )

    small_plane[mine] = small_mine[...]
    for i, s in pieces[1:]:
        sum_copy(i, s).start()

    all_pass(1, grad_all)
    all_end(1, grad_all)
    for a in range(TAPS):
        first[a] = penalty_weight * correlate(0, grad_all, a)

    slice_end(1)
    inner, outer = lax.rem(me["tm"], line), me["tm"] // line

    def along(step):
        return lax.rem(inner + step, line)

    def part_copy(a, step):
        at = a * line + step
        return remote(
            code.at[a, along(step)], land.at[a, inner], part_send.at[at], part_recv.at[at],
            device(tm=outer * line + along(step)),
        )

    def scatter(a):
        both = (first[a] + correlate(1, clip_all, a)).reshape(taps, share, chans)
        for t in range(line):
            total[a, t] = both[:, t * part : (t + 1) * part]
        for step in range(1, line):
            value, top = encode(total[a, along(step)])
            code[a, along(step), pl.ds(0, taps)] = value
            code[a, along(step), taps] = top
            part_copy(a, step).start()

    groups = tm // line

    def more_copy(a, step):
        at = a * groups + step
        spot = lax.rem(outer + step, groups)
        return remote(
            more.at[a, outer], more.at[a, outer], more_send.at[at], more_recv.at[at],
            device(tm=spot * line + inner),
        )

    def line_copy(a, step):
        at = a * line + step
        block = full.at[a, mine, inner]
        return remote(
            block, block, line_send.at[at], line_recv.at[at],
            device(tm=outer * line + along(step)),
        )

    def collect(a):
        value = total[a, inner]
        for step in range(1, line):
            part_copy(a, step).wait()
        for step in range(1, line):
            value = value + decode(land[a, along(step)], taps)
        if groups > 1:
            value, top = encode(value)
            more[a, outer, pl.ds(0, taps)] = value
            more[a, outer, taps] = top
            for step in range(1, groups):
                more_copy(a, step).start()
            for step in range(1, groups):
                more_copy(a, step).wait()
            value = decode(more[a, 0], taps)
            for k in range(1, groups):
                value = value + decode(more[a, k], taps)
        value, top = encode(value)
        full[a, mine, inner, pl.ds(0, taps)] = value
        full[a, mine, inner, taps] = top
        for step in range(1, line):
            line_copy(a, step).start()

    half = line // 2
    sides = [("rows", s) for s in range(1, near)] + [("dp", i) for i in range(1, dp)]

    def go(side):
        axis, step = side
        return {axis: shift(axis, step * (pair if axis == "rows" else 1))}

    def come(side):
        axis, step = side
        return {axis: shift(axis, -step * (pair if axis == "rows" else 1))}

    def number(place):
        place = dict(me, **place)
        return place["dp"] * rows + place["rows"]

    def near_copy(a, side):
        at = a * len(sides) + sides.index(side)
        block = full.at[a, mine]
        return remote(block, block, near_send.at[at], near_recv.at[at], device(**go(side)))

    turns = []
    for one in sides:
        for two in sides:
            if one[0] == two[0]:
                continue
            rest = (0, half) if one[0] == "rows" else (half, line - half)
            if rest[1]:
                turns.append((one, two, rest))

    def turn_copy(a, turn):
        one, two, rest = turn
        at = a * len(turns) + turns.index(turn)
        block = full.at[a, number(come(one)), pl.ds(*rest)]
        return remote(block, block, turn_send.at[at], turn_recv.at[at], device(**go(two)))

    hops = [(None, None)] + [(side, None) for side in sides] + turns

    def pair_copy(a, k):
        at = a * len(hops) + k
        if k == 0:
            block = full.at[a, mine]
        elif k <= len(sides):
            block = full.at[a, number(come(hops[k][0]))]
        else:
            one, two, rest = hops[k]
            block = full.at[a, number(dict(come(one), **come(two))), pl.ds(*rest)]
        return remote(block, block, pair_send.at[at], pair_recv.at[at], device(rows=partner))

    def spread(a):
        for step in range(1, line):
            line_copy(a, step).wait()
        for side in sides:
            near_copy(a, side).start()
        if pair == 2:
            pair_copy(a, 0).start()

    def relay(a):
        for k, side in enumerate(sides):
            near_copy(a, side).wait()
            for turn in turns:
                if turn[0] == side:
                    turn_copy(a, turn).start()
            if pair == 2:
                pair_copy(a, 1 + k).start()

    def handover(a):
        for k, turn in enumerate(turns):
            turn_copy(a, turn).wait()
            if pair == 2:
                pair_copy(a, 1 + len(sides) + k).start()

    def finish(a):
        if pair == 2:
            for k in range(len(hops)):
                pair_copy(a, k).wait()
        per = LANES // part

        def tap(k, carry):
            for high in range(chans // LANES):
                for low in range(chans // LANES):
                    at = low * LANES
                    pile = []
                    for n in range(high * per, (high + 1) * per):
                        block = full.at[a, n // line, n % line]
                        unit = block[taps, :, at : at + LANES].astype(jnp.float32)
                        value = jnp.log(block[k, :, at : at + LANES].astype(jnp.float32))
                        pile.append(value * (unit * (1.0 / (SPAN * math.log(2.0)))))
                    out_ref[a * taps + k, at : at + LANES, high * LANES : (high + 1) * LANES] = (
                        jnp.concatenate(pile, axis=0).T
                    )
            return carry

        lax.fori_loop(0, taps, tap, 0)

    def end_copy(step):
        return remote(
            small_mine, small_line.at[me["tm"]], end_send.at[step], end_recv.at[step],
            device(tm=shift("tm", step)),
        )

    def small_middle():
        for i, s in pieces[1:]:
            sum_copy(i, s).wait()
        small_mine[...] = jnp.sum(small_plane[...], axis=0)
        small_line[me["tm"]] = small_mine[...]
        for step in range(1, tm):
            end_copy(step).start()

    def small_end():
        for step in range(1, tm):
            end_copy(step).wait()
        value = jnp.sum(small_line[...], axis=0)
        bias_out[...] = value[0:1]
        head_out[...] = value[1:2]

    stages = (scatter, collect, spread, relay, handover, finish)
    for wave in range(len(stages) + TAPS - 1):
        for a in range(TAPS):
            level = wave - a
            if 0 <= level < len(stages):
                stages[level](a)
        if wave == 0:
            small_middle()
        if wave == 3:
            small_end()


def per_device(sizes, clips, weight, bias, head):
    dp, tm, rows = sizes
    _, frames, _, cols, chans = clips.shape
    count = frames * cols
    plane = dp * rows
    share = chans // plane
    line, groups = split_line(tm, share // SUB)
    part = share // line
    taps = TAPS**2
    pair = 2 if rows % 2 == 0 else 1
    near = rows // pair
    close = dp * near - 1
    sides = near - 1 + dp - 1
    turns = 2 * (near - 1) * (dp - 1)
    pad = pltpu.VMEM((frames + 2, 3, cols, chans), jnp.bfloat16)
    field = pltpu.VMEM((count, chans), jnp.float32)
    gathered = pltpu.VMEM((plane, count, chans), jnp.bfloat16)
    coded = pltpu.VMEM((TAPS, line, taps + 1, part, chans), jnp.bfloat16)

    def dma(n):
        return pltpu.SemaphoreType.DMA((max(n, 1),))

    sems = []
    for n in (
        24, 2 * close, 2 * (close + 1), 6 * plane, TAPS * line, TAPS * groups,
        TAPS * line, TAPS * sides, TAPS * turns, TAPS * (1 + sides + turns), plane, tm,
    ):
        sems += [dma(n), dma(n)]
    vmem = pl.BlockSpec(memory_space=pltpu.VMEM)
    hbm = pl.BlockSpec(memory_space=pl.ANY)
    grad_weight, grad_bias, grad_head = pl.pallas_call(
        functools.partial(kernel, sizes, line),
        out_shape=(
            pltpu.VMEM((TAPS**3, chans, chans), jnp.float32),
            pltpu.VMEM((1, chans), jnp.float32),
            pltpu.VMEM((1, chans), jnp.float32),
        ),
        in_specs=[hbm, hbm, vmem, vmem],
        out_specs=(vmem, vmem, vmem),
        scratch_shapes=[
            pltpu.VMEM((TAPS**3, chans, chans), jnp.bfloat16),
            pad, pad, pad,
            pltpu.VMEM((TAPS, count, chans), jnp.float32),
            field, field,
            gathered, gathered,
            pltpu.VMEM((2, frames, chans, cols), jnp.bfloat16),
            pltpu.VMEM((2, plane, frames + 2, share, cols), jnp.bfloat16),
            pltpu.VMEM((2, dp, rows + 2, frames + 2, TAPS * share, cols), jnp.bfloat16),
            pltpu.VMEM((TAPS, taps * share, chans), jnp.float32),
            pltpu.VMEM((TAPS, line, taps, part, chans), jnp.float32),
            coded, coded,
            pltpu.VMEM((TAPS, groups, taps + 1, part, chans), jnp.bfloat16),
            pltpu.VMEM((TAPS, plane, line, taps + 1, part, chans), jnp.bfloat16),
            pltpu.VMEM((SUB, chans), jnp.float32),
            pltpu.VMEM((plane, SUB, chans), jnp.float32),
            pltpu.VMEM((tm, SUB, chans), jnp.float32),
            dma(2), *sems,
        ],
        compiler_params=pltpu.CompilerParams(
            collective_id=0, has_side_effects=True, vmem_limit_bytes=48 * 1024 * 1024
        ),
    )(
        pltpu.with_memory_space_constraint(clips.reshape(frames, cols, chans), pltpu.HBM),
        weight.reshape(TAPS**3, chans, chans),
        bias.reshape(1, chans),
        head.reshape(1, chans),
    )
    grad_weight = grad_weight.reshape(TAPS, TAPS, TAPS, chans, chans)
    return grad_weight, grad_bias.reshape(chans), grad_head.reshape(chans)


def solution(mesh):
    sizes = tuple(mesh.shape[axis] for axis in ("dp", "tm", "rows"))
    return jax.shard_map(
        functools.partial(per_device, sizes),
        mesh=mesh,
        in_specs=(P("dp", "tm", "rows", None, None), P(), P(), P()),
        out_specs=(P(), P(), P()),
        check_vma=False,
    )
```

```python
import functools
import math

import jax
import jax.numpy as jnp
from jax import lax
from jax.experimental import pallas as pl
from jax.experimental.pallas import tpu as pltpu
from jax.sharding import PartitionSpec as P

penalty_weight = 0.01
MESH = pl.DeviceIdType.MESH
SUB = 8
TAPS = 3
SPAN = 120.0
LANES = 128
WIDE = 128


def split_line(tm, most):
    line = 1
    while tm % (2 * line) == 0 and 2 * line <= most:
        line *= 2
    return line, tm // line


def decode(block, taps):
    unit = block[taps].astype(jnp.float32) * (1.0 / (SPAN * math.log(2.0)))
    return jnp.log(block[:taps].astype(jnp.float32)) * unit[None]


def encode(value):
    top = (jnp.max(jnp.abs(value), axis=0) * 1.01 + 1e-30).astype(jnp.bfloat16)
    rate = SPAN / top.astype(jnp.float32)
    return jnp.exp2(value * rate[None]).astype(jnp.bfloat16), top


def kernel(
    sizes, line, clips_ref, weight_ref, bias_ref, head_ref,
    out_ref, bias_out, head_out,
    w_ref, wt_ref, clip_pad, score_pad, grad_pad, acc, slope_ref, curve_ref,
    clip_all, grad_all, turned, slices, shifts, first, total, code, land, more, full,
    small_mine, small_plane, small_line,
    local_sem, halo_send, halo_recv, hand_send, hand_recv, all_send, all_recv, pass_send, pass_recv,
    slice_send, slice_recv, part_send, part_recv, more_send, more_recv,
    line_send, line_recv, near_send, near_recv, turn_send, turn_recv, pair_send, pair_recv,
    sum_send, sum_recv, end_send, end_recv,
):
    dp, tm, rows = sizes
    frames, cols, chans = clips_ref.shape
    count = frames * cols
    plane = dp * rows
    share = chans // plane
    part = share // line
    taps = TAPS**2
    pair = 2 if rows % 2 == 0 else 1
    near = rows // pair
    me = {"dp": lax.axis_index("dp"), "tm": lax.axis_index("tm"), "rows": lax.axis_index("rows")}
    mine = me["dp"] * rows + me["rows"]

    def device(**moved):
        place = dict(me, **moved)
        return (place["dp"], place["tm"], place["rows"])

    def shift(axis, step):
        return lax.rem(me[axis] + step % dict(dp=dp, tm=tm, rows=rows)[axis], dict(dp=dp, tm=tm, rows=rows)[axis])

    def remote(src, dst, send, recv, target):
        return pltpu.make_async_remote_copy(
            src_ref=src, dst_ref=dst, send_sem=send, recv_sem=recv,
            device_id=target, device_id_type=MESH,
        )

    weight_copy = pltpu.make_async_copy(weight_ref, w_ref, local_sem.at[0])
    weight_copy.start()
    clip_copy = pltpu.make_async_copy(
        clips_ref, clip_pad.at[pl.ds(1, frames), 1], local_sem.at[1]
    )
    clip_copy.start()
    keep_copy = pltpu.make_async_copy(clips_ref, clip_all.at[mine], local_sem.at[2])
    keep_copy.start()

    steps = {(i, t % tm, s) for i in range(dp) for t in (-1, 0, 1) for s in range(rows)}
    steps |= {(0, t, 0) for t in range(tm)}
    steps = sorted(steps - {(0, 0, 0)})
    barrier = pltpu.get_barrier_semaphore()
    for i, t, s in steps:
        pl.semaphore_signal(
            barrier, inc=1, device_id=(shift("dp", i), shift("tm", t), shift("rows", s)),
            device_id_type=MESH,
        )
    for axis, bound, fill in (
        ("rows", 0, lambda pad: pad.at[:, 0]), ("rows", rows - 1, lambda pad: pad.at[:, 2]),
        ("tm", 0, lambda pad: pad.at[0]), ("tm", tm - 1, lambda pad: pad.at[frames + 1]),
    ):
        @pl.when(me[axis] == bound)
        def _():
            for pad in (clip_pad, score_pad, grad_pad):
                at = fill(pad)
                at[...] = jnp.zeros(at.shape, at.dtype)
    for which in range(2):
        for edge in (0, rows + 1):
            shifts[which, :, edge] = jnp.zeros(shifts.shape[1:2] + shifts.shape[3:], shifts.dtype)
        for edge, bound in ((0, 0), (frames + 1, tm - 1)):
            @pl.when(me["tm"] == bound)
            def _():
                slices[which, :, edge] = jnp.zeros((plane, share, cols), slices.dtype)
    pl.semaphore_wait(barrier, len(steps))

    moves = [(t, r) for t in (-1, 0, 1) for r in (-1, 0, 1) if (t, r) != (0, 0)]
    partner = me["rows"] + 1 - 2 * lax.rem(me["rows"], 2) if pair == 2 else me["rows"]
    mirror = rows - 1 - me["rows"]
    toward = partner - me["rows"]

    def inside(t, r):
        ok = None
        for axis, step, size in (("tm", t, tm), ("rows", r, rows)):
            if step:
                cond = me[axis] > 0 if step < 0 else me[axis] < size - 1
                ok = cond if ok is None else jnp.logical_and(ok, cond)
        return ok

    def leaves(t, r, sender):
        ok = inside(t, r) if sender else inside(-t, -r)
        if pair == 1:
            return ok
        row = me["rows"] if sender else me["rows"] - r
        return jnp.logical_and(ok, lax.rem(row, 2) == (0 if r < 0 else 1))

    def halo_copy(which, pad, source, t, r):
        slot = which * len(moves) + moves.index((t, r))
        if t == 0:
            here, there = pl.ds(0, frames), pl.ds(1, frames)
        elif t > 0:
            here, there = pl.ds(frames - 1, 1), pl.ds(0, 1)
        else:
            here, there = pl.ds(0, 1), pl.ds(frames + 1, 1)
        return remote(
            source.at[here], pad.at[there, 1 - r], halo_send.at[slot], halo_recv.at[slot],
            device(tm=me["tm"] + t, rows=me["rows"] + r),
        )

    def hand_copy(which, pad, t):
        at = 2 * which + (t > 0)
        edge = 0 if t > 0 else frames + 1
        return remote(
            pad.at[edge, 1], pad.at[edge, 1 - toward], hand_send.at[at], hand_recv.at[at],
            device(rows=partner),
        )

    def depth_start(which, pad, source):
        for t in (-1, 1):
            @pl.when(inside(t, 0))
            def _():
                halo_copy(which, pad, source, t, 0).start()

    def side_start(which, pad, source):
        for r in (-1, 1):
            @pl.when(inside(0, r))
            def _():
                halo_copy(which, pad, source, 0, r).start()

    def corner_start(which, pad, source):
        for t in (-1, 1):
            for r in (-1, 1):
                @pl.when(leaves(t, r, True))
                def _():
                    halo_copy(which, pad, source, t, r).start()

    def side_sent(which, pad, source):
        for r in (-1, 1):
            @pl.when(inside(0, r))
            def _():
                halo_copy(which, pad, source, 0, r).wait_send()

    def side_wait(which, pad, source):
        for r in (-1, 1):
            @pl.when(inside(0, -r))
            def _():
                halo_copy(which, pad, source, 0, r).wait_recv()

    def depth_wait(which, pad, source):
        for t in (-1, 1):
            @pl.when(inside(-t, 0))
            def _():
                halo_copy(which, pad, source, t, 0).wait_recv()
                if pair == 2:
                    hand_copy(which, pad, t).start()
        for t in (-1, 1):
            @pl.when(inside(t, 0))
            def _():
                halo_copy(which, pad, source, t, 0).wait_send()

    def corner_wait(which, pad, source):
        for t in (-1, 1):
            for r in (-1, 1):
                @pl.when(leaves(t, r, True))
                def _():
                    halo_copy(which, pad, source, t, r).wait_send()

                @pl.when(leaves(t, r, False))
                def _():
                    halo_copy(which, pad, source, t, r).wait_recv()
            if pair == 2:
                @pl.when(inside(-t, 0))
                def _():
                    hand_copy(which, pad, t).wait()

    column = lax.rem(lax.broadcasted_iota(jnp.int32, (count, chans), 0), cols)

    def earlier(value):
        return jnp.where(column == 0, 0.0, pltpu.roll(value, 1, 0))

    def later(value):
        return jnp.where(column == cols - 1, 0.0, pltpu.roll(value, count - 1, 0))

    def conv(which, pad, source, kernel_ref, idle, sent, side, between):
        def put(shift_f, start, many, places, new=False):
            if not many:
                return
            left = jnp.concatenate(
                [
                    pad[pl.ds(start + shift_f, many), b].reshape(many * cols, chans)
                    for b in places
                ],
                axis=1,
            )
            at = pl.ds(start * cols, many * cols)
            for d in range(TAPS):
                taps = [kernel_ref[(shift_f * TAPS + b) * TAPS + d] for b in places]
                value = jnp.dot(
                    left, jnp.concatenate(taps, axis=0), preferred_element_type=jnp.float32
                )
                acc[d, at] = value if new else acc[d, at] + value

        def inner_frames(places, new):
            put(1, 0, frames, places, new)
            put(0, 1, frames - 1, places)
            put(2, 0, frames - 1, places)

        def outer_frames(places):
            put(0, 0, 1, places)
            put(2, frames - 1, 1, places)

        inner_frames((1,), True)
        corner_start(which, pad, source)
        idle()
        side(which, pad, source)
        inner_frames((0, 2), False)
        depth_wait(which, pad, source)
        between()
        outer_frames((1,))
        corner_wait(which, pad, source)
        outer_frames((0, 2))
        sent()
        return earlier(acc[0]) + acc[1] + later(acc[2])

    others = range(1, dp)
    across = [(0, 0)] + [(i, 0) for i in others]
    if near == 2:
        across = [(0, 0), (0, 1)] + [(i, 0) for i in others] + [(i, 1) for i in others]

    edge = jnp.logical_and(me["rows"] > 0, me["rows"] < rows - 1)

    def spot(i, m):
        return shift("dp", -i) * rows + (mirror if m else me["rows"])

    def all_copy(which, buf, i, m):
        at = which * len(across) + across.index((i, m))
        if i == 0:
            block, there = buf.at[mine], device(rows=mirror)
        else:
            block, there = buf.at[spot(0, m)], device(dp=shift("dp", i))
        return remote(block, block, all_send.at[at], all_recv.at[at], there)

    def pass_copy(which, buf, i, m):
        at = which * len(across) + across.index((i, m))
        block = buf.at[spot(i, m)]
        return remote(block, block, pass_send.at[at], pass_recv.at[at], device(rows=partner))

    def all_start(which, buf):
        if pair == 2:
            pass_copy(which, buf, 0, 0).start()
        if near == 2:
            @pl.when(edge)
            def _():
                all_copy(which, buf, 0, 1).start()

    def all_down(which, buf):
        for i in others:
            all_copy(which, buf, i, 0).start()

    def all_side(buf):
        def side(which, pad, source):
            at = which // 2
            if pair == 2:
                pass_copy(at, buf, 0, 0).wait_recv()
                pad[pl.ds(1, frames), 1 + toward] = buf[me["dp"] * rows + partner]
            if near == 2:
                @pl.when(edge)
                def _():
                    all_copy(at, buf, 0, 1).wait_recv()
                    pad[pl.ds(1, frames), 1 - toward] = buf[me["dp"] * rows + mirror]

        return side

    def all_sent(which, buf):
        if near == 2:
            @pl.when(edge)
            def _():
                all_copy(which, buf, 0, 1).wait_send()

    def relay_start(which, buf):
        for i in others:
            all_copy(which, buf, i, 1).start()
        pass_copy(which, buf, 0, 1).start()

    def all_between(which, buf):
        if near == 2:
            @pl.when(edge)
            def _():
                relay_start(which, buf)

            @pl.when(jnp.logical_not(edge))
            def _():
                all_copy(which, buf, 0, 1).start()

    def all_relay(which, buf):
        if near == 2:
            @pl.when(jnp.logical_not(edge))
            def _():
                all_copy(which, buf, 0, 1).wait_recv()
                relay_start(which, buf)

    def all_near(which, buf):
        if near == 2:
            pass_copy(which, buf, 0, 1).wait_recv()

    def all_far(which, buf, m):
        if m and near != 2:
            return
        for i in others:
            all_copy(which, buf, i, m).wait_recv()
            if pair == 2:
                pass_copy(which, buf, i, m).start()

    def all_end(which, buf):
        for i, m in across:
            if (i, m) == (0, 1):
                @pl.when(jnp.logical_not(edge))
                def _():
                    all_copy(which, buf, i, m).wait_send()
            elif i:
                all_copy(which, buf, i, m).wait_send()
            if pair == 2:
                pass_copy(which, buf, i, m).wait_send()
                if i:
                    pass_copy(which, buf, i, m).wait_recv()

    def slice_copy(which, t, i, s):
        at = which * 3 + t + 1
        y, r = shift("dp", i), shift("rows", s)
        rest = pl.ds(pl.multiple_of((y * rows + r) * share, share), share)
        if t == 0:
            src, dst = turned.at[which, :, rest], slices.at[which, mine, pl.ds(1, frames)]
        elif t > 0:
            src, dst = turned.at[which, frames - 1, rest], slices.at[which, mine, 0]
        else:
            src, dst = turned.at[which, 0, rest], slices.at[which, mine, frames + 1]
        return remote(
            src, dst, slice_send.at[at], slice_recv.at[at],
            device(dp=y, rows=r, tm=me["tm"] + t),
        )

    pieces = [(i, s) for i in range(dp) for s in range(rows)]

    def slice_start(which, value):
        for f in range(frames):
            turned[which, f] = value[f].T.astype(jnp.bfloat16)
        for t in (1, -1):
            @pl.when(inside(t, 0))
            def _():
                for i, s in pieces:
                    slice_copy(which, t, i, s).start()
        for i, s in pieces[1:]:
            slice_copy(which, 0, i, s).start()
        own = pl.ds(pl.multiple_of(mine * share, share), share)
        for f in range(frames):
            slices[which, mine, f + 1] = turned[which, f, own]

    lane = lax.broadcasted_iota(jnp.int32, (share, cols), 1)

    def slice_end(which):
        def whole(t):
            at = which * 3 + t + 1
            block = slices.at[which, :, 0] if t else slices.at[
                which, pl.ds(0, plane - 1), pl.ds(1, frames)
            ]
            return remote(block, block, slice_send.at[at], slice_recv.at[at], device())

        for t in (1, -1):
            @pl.when(inside(t, 0))
            def _():
                whole(t).wait_send()

            @pl.when(inside(-t, 0))
            def _():
                whole(t).wait_recv()
        whole(0).wait()
        for j in range(plane):
            for f in range(frames + 2):
                value = slices[which, j, f].astype(jnp.float32)
                after = jnp.where(lane == cols - 1, 0.0, pltpu.roll(value, cols - 1, 1))
                before = jnp.where(lane == 0, 0.0, pltpu.roll(value, 1, 1))
                shifts[which, j // rows, j % rows + 1, f] = jnp.concatenate(
                    [after, value, before], axis=0
                ).astype(jnp.bfloat16)

    def correlate(which, buf, a, clips):
        left = jnp.concatenate(
            [
                jnp.concatenate(
                    [
                        shifts[which, y, r + 2 - b, f + 2 - a]
                        for y in clips for r in range(rows) for f in range(frames)
                    ],
                    axis=1,
                )
                for b in range(TAPS)
            ],
            axis=0,
        )
        right = jnp.concatenate(
            [buf[pl.ds(y * rows, rows)].reshape(rows * count, chans) for y in clips], axis=0
        )
        return jnp.dot(left, right, preferred_element_type=jnp.float32)

    def turn_weight():
        def one(k, carry):
            wt_ref[TAPS**3 - 1 - k] = w_ref[k].T
            return carry

        lax.fori_loop(0, TAPS**3, one, 0, unroll=3)

    depth_start(0, clip_pad, clips_ref)
    clip_copy.wait()
    keep_copy.wait()
    all_start(0, clip_all)
    all_down(0, clip_all)
    weight_copy.wait()
    pre = bias_ref[...] + conv(
        0, clip_pad, clips_ref, w_ref, turn_weight, lambda: all_sent(0, clip_all),
        all_side(clip_all), lambda: all_between(0, clip_all),
    )
    sig = jax.nn.sigmoid(pre)
    slope = sig * (1.0 + pre * (1.0 - sig))
    slope_ref[...] = slope
    curve_ref[...] = sig * (1.0 - sig) * (2.0 + pre * (1.0 - 2.0 * sig))
    score = (head_ref[...] * slope).astype(jnp.bfloat16)
    score_pad[pl.ds(1, frames), 1] = score.reshape(frames, cols, chans)
    score_own = score_pad.at[pl.ds(1, frames), 1]
    depth_start(1, score_pad, score_own)
    side_start(1, score_pad, score_own)
    all_relay(0, clip_all)
    all_far(0, clip_all, 0)

    input_grad = conv(
        1, score_pad, score_own, wt_ref, lambda: None,
        lambda: side_sent(1, score_pad, score_own), side_wait,
        lambda: slice_start(0, score_pad[pl.ds(1, frames), 1].astype(jnp.float32)),
    ).astype(jnp.bfloat16).reshape(frames, cols, chans)
    grad_pad[pl.ds(1, frames), 1] = input_grad
    grad_all[mine] = input_grad
    grad_own = grad_pad.at[pl.ds(1, frames), 1]
    depth_start(2, grad_pad, grad_own)
    all_start(1, grad_all)
    all_down(1, grad_all)
    all_far(0, clip_all, 1)

    back = penalty_weight * conv(
        2, grad_pad, grad_own, w_ref, lambda: None, lambda: all_sent(1, grad_all),
        all_side(grad_all), lambda: all_between(1, grad_all),
    )
    pre_grad = back * head_ref[...] * curve_ref[...]
    slice_start(
        1, pre_grad.astype(jnp.bfloat16).astype(jnp.float32).reshape(frames, cols, chans)
    )
    small_mine[...] = jnp.zeros_like(small_mine)
    small_mine[pl.ds(0, 1)] = jnp.sum(pre_grad, axis=0, keepdims=True)
    small_mine[pl.ds(1, 1)] = jnp.sum(back * slope_ref[...], axis=0, keepdims=True)

    def sum_copy(i, s):
        return remote(
            small_mine, small_plane.at[mine], sum_send.at[0], sum_recv.at[0],
            device(dp=shift("dp", i), rows=shift("rows", s)),
        )

    small_plane[mine] = small_mine[...]
    for i, s in pieces[1:]:
        sum_copy(i, s).start()

    slice_end(0)
    all_relay(1, grad_all)
    all_far(1, grad_all, 0)
    all_near(0, clip_all)
    all_end(0, clip_all)
    all_near(1, grad_all)
    for a in range(TAPS):
        first[a] = correlate(0, grad_all, a, [me["dp"]])
    all_far(1, grad_all, 1)
    all_end(1, grad_all)
    for a in range(TAPS):
        first[a] = penalty_weight * (
            first[a] + correlate(0, grad_all, a, [shift("dp", i) for i in others])
            if dp > 1 else first[a]
        )

    slice_end(1)
    inner, outer = lax.rem(me["tm"], line), me["tm"] // line
    wide = full.shape[-1]
    chunks = [(a, low) for a in range(TAPS) for low in range(chans // wide)]

    def along(step):
        return lax.rem(inner + step, line)

    def part_copy(c, step):
        return remote(
            code.at[c, along(step)], land.at[c, inner], part_send.at[c], part_recv.at[c],
            device(tm=outer * line + along(step)),
        )

    def part_all(c):
        block = land.at[c, pl.ds(0, line - 1)]
        return remote(block, block, part_send.at[c], part_recv.at[c], device())

    def scatter(c):
        a, low = chunks[c]
        if low == 0:
            both = (first[a] + correlate(1, clip_all, a, range(dp))).reshape(taps, share, chans)
            for k in range(chans // wide):
                for t in range(line):
                    total[c + k, t] = both[
                        :, t * part : (t + 1) * part, k * wide : (k + 1) * wide
                    ]
        for step in range(line - 1, 0, -1):
            value, top = encode(total[c, along(step)])
            code[c, along(step), pl.ds(0, taps)] = value
            code[c, along(step), taps] = top
        if c > 1 and line > 1:
            part_all(c - 2).wait_send()
        for step in range(line - 1, 0, -1):
            part_copy(c, step).start()

    groups = tm // line

    def more_copy(c, step):
        spot = lax.rem(outer + step, groups)
        return remote(
            more.at[c, outer], more.at[c, outer], more_send.at[c], more_recv.at[c],
            device(tm=spot * line + inner),
        )

    upper = inner // 2
    ranks = [inner, inner + 1 - 2 * lax.rem(inner, 2), 2 - upper, 3 - 3 * upper][:line]
    middle = lax.rem(inner + upper, 2) == 1

    def line_copy(c, rank, to):
        here = full.at[c, mine * line + ranks[rank]]
        return remote(
            here, here, line_send.at[c], line_recv.at[c * line + ranks[rank]],
            device(tm=outer * line + to),
        )

    def collect(c):
        value = total[c, inner]
        if line > 1:
            part_all(c).wait_recv()
            if c >= len(chunks) - 2:
                part_all(c).wait_send()
        for step in range(1, line):
            value = value + decode(land[c, along(step)], taps)
        if groups > 1:
            value, top = encode(value)
            more[c, outer, pl.ds(0, taps)] = value
            more[c, outer, taps] = top
            for step in range(1, groups):
                more_copy(c, step).start()
            block = more.at[c, pl.ds(0, groups - 1)]
            remote(block, block, more_send.at[c], more_recv.at[c], device()).wait()
            value = decode(more[c, 0], taps)
            for k in range(1, groups):
                value = value + decode(more[c, k], taps)
        value, top = encode(value)
        full[c, mine * line + inner, pl.ds(0, taps)] = value
        full[c, mine * line + inner, taps] = top
        for rank in range(min(line - 1, 2), 0, -1):
            line_copy(c, 0, ranks[rank]).start()
        share_out(c, 0)

    def share_out(c, rank):
        for side in sides:
            near_copy(c, rank, side).start()
        if pair == 2:
            pair_copy(c, rank, 0).start()

    def take(c, rank):
        line_copy(c, rank, inner).wait_recv()
        if rank > 1:
            @pl.when(middle)
            def _():
                line_copy(c, rank, ranks[1]).start()
        share_out(c, rank)

    sides = [("rows", s) for s in range(1, near)] + [("dp", i) for i in range(1, dp)]

    def go(side):
        axis, step = side
        return {axis: shift(axis, step * (pair if axis == "rows" else 1))}

    def come(side):
        axis, step = side
        return {axis: shift(axis, -step * (pair if axis == "rows" else 1))}

    def number(place):
        place = dict(me, **place)
        return place["dp"] * rows + place["rows"]

    turns = [(one, two) for one in sides for two in sides if one[0] != two[0]]
    hops = [()] + [(side,) for side in sides] + turns

    def block_at(c, rank, hop):
        place = {}
        for side in hop:
            place.update(come(side))
        return full.at[c, number(place) * line + ranks[rank]]

    def turned_by(rank):
        return [turn for turn in turns if turn[0][0] == ("dp" if rank % 2 else "rows")]

    per_turn = max(1, len(turns) // 2)

    def near_copy(c, rank, side):
        at = (c * line + rank) * len(sides) + sides.index(side)
        block = block_at(c, rank, ())
        return remote(block, block, near_send.at[c], near_recv.at[at], device(**go(side)))

    def turn_copy(c, rank, turn):
        at = (c * line + rank) * per_turn + turned_by(rank).index(turn)
        block = block_at(c, rank, turn[:1])
        return remote(block, block, turn_send.at[c], turn_recv.at[at], device(**go(turn[1])))

    def pair_copy(c, rank, k):
        block = block_at(c, rank, hops[k])
        return remote(block, block, pair_send.at[c], pair_recv.at[c], device(rows=partner))

    def relay(c, rank):
        for k, side in enumerate(sides):
            near_copy(c, rank, side).wait_recv()
            for turn in turned_by(rank):
                if turn[0] == side:
                    turn_copy(c, rank, turn).start()
            if pair == 2:
                pair_copy(c, rank, 1 + k).start()

    def handover(c, rank):
        for turn in turned_by(rank):
            turn_copy(c, rank, turn).wait_recv()
            if pair == 2:
                pair_copy(c, rank, hops.index(turn)).start()

    def finish(c):
        a, low = chunks[c]
        ended = [(near_send, line * len(sides)), (turn_send, sum(len(turned_by(k)) for k in range(line)))]
        for sem, n in ended + [(line_send, min(line - 1, 2))]:
            if n:
                block = full.at[c, pl.ds(0, n)]
                remote(block, block, sem.at[c], sem.at[c], device()).wait_send()
        if line == 4:
            @pl.when(middle)
            def _():
                block = full.at[c, pl.ds(0, 2)]
                remote(block, block, line_send.at[c], line_send.at[c], device()).wait_send()
        if pair == 2:
            block = full.at[c, pl.ds(0, plane * line // 2)]
            remote(block, block, pair_send.at[c], pair_recv.at[c], device()).wait()
        per = LANES // part

        def tap(k, carry):
            for high in range(chans // LANES):
                for left in range(0, wide, LANES):
                    pile = []
                    for n in range(high * per, (high + 1) * per):
                        block = full.at[c, n]
                        unit = block[taps, :, left : left + LANES].astype(jnp.float32)
                        value = jnp.log(block[k, :, left : left + LANES].astype(jnp.float32))
                        pile.append(value * (unit * (1.0 / (SPAN * math.log(2.0)))))
                    out_ref[
                        a * taps + k, low * wide + left : low * wide + left + LANES,
                        high * LANES : (high + 1) * LANES,
                    ] = jnp.concatenate(pile, axis=0).T
            return carry

        lax.fori_loop(0, taps, tap, 0, unroll=True)

    def end_copy(step):
        return remote(
            small_mine, small_line.at[me["tm"]], end_send.at[0], end_recv.at[0],
            device(tm=shift("tm", step)),
        )

    def small_middle():
        block = small_plane.at[pl.ds(0, plane - 1)]
        if plane > 1:
            remote(block, block, sum_send.at[0], sum_recv.at[0], device()).wait()
        small_mine[...] = jnp.sum(small_plane[...], axis=0)
        small_line[me["tm"]] = small_mine[...]
        for step in range(1, tm):
            end_copy(step).start()

    def small_end():
        block = small_line.at[pl.ds(0, tm - 1)]
        if tm > 1:
            remote(block, block, end_send.at[0], end_recv.at[0], device()).wait()
        value = jnp.sum(small_line[...], axis=0)
        bias_out[...] = value[0:1]
        head_out[...] = value[1:2]

    pace = 1.77 * wide / LANES
    order = [(4.0, small_middle, ()), (16.0, small_end, ())]
    for c in range(len(chunks)):
        got = 2.9 + pace + pace * c
        order += [(pace * max(c - 1, 0), scatter, (c,)), (got, collect, (c,))]
        for rank in range(line):
            here = got + (0.0, 3.5, 5.0, 6.5)[rank]
            if rank:
                order.append((here, take, (c, rank)))
            order += [(here + 3.5, relay, (c, rank)), (here + 7.5, handover, (c, rank))]
        order.append((got + 16.5, finish, (c,)))
    for _, stage, what in sorted(order, key=lambda entry: entry[0]):
        stage(*what)


def per_device(sizes, clips, weight, bias, head):
    dp, tm, rows = sizes
    _, frames, _, cols, chans = clips.shape
    count = frames * cols
    plane = dp * rows
    share = chans // plane
    line, groups = split_line(tm, share // SUB)
    part = share // line
    taps = TAPS**2
    pair = 2 if rows % 2 == 0 else 1
    near = rows // pair
    if rows not in (1, 2, 4):
        raise ValueError("rows")
    sides = near - 1 + dp - 1
    turns = 2 * (near - 1) * (dp - 1)
    pad = pltpu.VMEM((frames + 2, 3, cols, chans), jnp.bfloat16)
    field = pltpu.VMEM((count, chans), jnp.float32)
    gathered = pltpu.VMEM((plane, frames, cols, chans), jnp.bfloat16)
    wide = WIDE if chans % WIDE == 0 else chans
    chunks = TAPS * (chans // wide)
    coded = pltpu.VMEM((chunks, line, taps + 1, part, wide), jnp.bfloat16)

    def dma(n):
        return pltpu.SemaphoreType.DMA((max(n, 1),))

    sems = []
    for send, recv in (
        (24, 24), (6, 6), (2 * dp * near, 2 * dp * near), (2 * dp * near, 2 * dp * near),
        (6, 6), (chunks, chunks),
        (chunks, chunks) if groups > 1 else (1, 1), (chunks, chunks * line),
        (chunks, chunks * line * sides), (chunks, chunks * line * max(1, turns // 2)),
        (chunks, chunks), (1, 1), (1, 1),
    ):
        sems += [dma(send), dma(recv)]
    vmem = pl.BlockSpec(memory_space=pltpu.VMEM)
    hbm = pl.BlockSpec(memory_space=pl.ANY)
    grad_weight, grad_bias, grad_head = pl.pallas_call(
        functools.partial(kernel, sizes, line),
        out_shape=(
            pltpu.VMEM((TAPS**3, chans, chans), jnp.float32),
            pltpu.VMEM((1, chans), jnp.float32),
            pltpu.VMEM((1, chans), jnp.float32),
        ),
        in_specs=[hbm, hbm, vmem, vmem],
        out_specs=(vmem, vmem, vmem),
        scratch_shapes=[
            pltpu.VMEM((TAPS**3, chans, chans), jnp.bfloat16),
            pltpu.VMEM((TAPS**3, chans, chans), jnp.bfloat16),
            pad, pad, pad,
            pltpu.VMEM((TAPS, count, chans), jnp.float32),
            field, field,
            gathered, gathered,
            pltpu.VMEM((2, frames, chans, cols), jnp.bfloat16),
            pltpu.VMEM((2, plane, frames + 2, share, cols), jnp.bfloat16),
            pltpu.VMEM((2, dp, rows + 2, frames + 2, TAPS * share, cols), jnp.bfloat16),
            pltpu.VMEM((TAPS, taps * share, chans), jnp.float32),
            pltpu.VMEM((chunks, line, taps, part, wide), jnp.float32),
            coded, coded,
            pltpu.VMEM((chunks, groups, taps + 1, part, wide), jnp.bfloat16),
            pltpu.VMEM((chunks, plane * line, taps + 1, part, wide), jnp.bfloat16),
            pltpu.VMEM((SUB, chans), jnp.float32),
            pltpu.VMEM((plane, SUB, chans), jnp.float32),
            pltpu.VMEM((tm, SUB, chans), jnp.float32),
            dma(3), *sems,
        ],
        compiler_params=pltpu.CompilerParams(
            collective_id=0, has_side_effects=True, vmem_limit_bytes=48 * 1024 * 1024
        ),
    )(
        pltpu.with_memory_space_constraint(clips.reshape(frames, cols, chans), pltpu.HBM),
        weight.reshape(TAPS**3, chans, chans),
        bias.reshape(1, chans),
        head.reshape(1, chans),
    )
    grad_weight = grad_weight.reshape(TAPS, TAPS, TAPS, chans, chans)
    return grad_weight, grad_bias.reshape(chans), grad_head.reshape(chans)


def solution(mesh):
    sizes = tuple(mesh.shape[axis] for axis in ("dp", "tm", "rows"))
    return jax.shard_map(
        functools.partial(per_device, sizes),
        mesh=mesh,
        in_specs=(P("dp", "tm", "rows", None, None), P(), P(), P()),
        out_specs=(P(), P(), P()),
        check_vma=False,
    )
```

```python
import functools
import math

import jax
import jax.numpy as jnp
from jax import lax
from jax.experimental import pallas as pl
from jax.experimental.pallas import tpu as pltpu
from jax.sharding import PartitionSpec as P

penalty_weight = 0.01
MESH = pl.DeviceIdType.MESH
SUB = 8
TAPS = 3
SPAN = 120.0
LANES = 128
WIDE = 128


def split_line(tm, most):
    line = 1
    while tm % (2 * line) == 0 and 2 * line <= most:
        line *= 2
    return line, tm // line


def decode(block, taps):
    unit = block[taps].astype(jnp.float32) * (1.0 / (SPAN * math.log(2.0)))
    return jnp.log(block[:taps].astype(jnp.float32)) * unit[None]


def encode(value):
    top = (jnp.max(jnp.abs(value), axis=0) * 1.01 + 1e-30).astype(jnp.bfloat16)
    rate = SPAN / top.astype(jnp.float32)
    return jnp.exp2(value * rate[None]).astype(jnp.bfloat16), top


def kernel(
    sizes, line, clips_ref, weight_ref, bias_ref, head_ref,
    out_ref, bias_out, head_out,
    w_ref, wt_ref, clip_pad, score_pad, grad_pad, acc, slope_ref, curve_ref,
    clip_all, grad_all, turned, slices, shifts, first, total, code, land, more, full,
    small_mine, small_plane, small_line,
    local_sem, halo_send, halo_recv, hand_send, hand_recv, all_send, all_recv, pass_send, pass_recv,
    slice_send, slice_recv, part_send, part_recv, more_send, more_recv,
    line_send, line_recv, near_send, near_recv, turn_send, turn_recv, pair_send, pair_recv,
    sum_send, sum_recv, end_send, end_recv,
):
    dp, tm, rows = sizes
    frames, cols, chans = clips_ref.shape
    count = frames * cols
    plane = dp * rows
    share = chans // plane
    part = share // line
    taps = TAPS**2
    pair = 2 if rows % 2 == 0 else 1
    near = rows // pair
    me = {"dp": lax.axis_index("dp"), "tm": lax.axis_index("tm"), "rows": lax.axis_index("rows")}
    mine = me["dp"] * rows + me["rows"]

    def device(**moved):
        place = dict(me, **moved)
        return (place["dp"], place["tm"], place["rows"])

    def shift(axis, step):
        return lax.rem(me[axis] + step % dict(dp=dp, tm=tm, rows=rows)[axis], dict(dp=dp, tm=tm, rows=rows)[axis])

    def remote(src, dst, send, recv, target):
        return pltpu.make_async_remote_copy(
            src_ref=src, dst_ref=dst, send_sem=send, recv_sem=recv,
            device_id=target, device_id_type=MESH,
        )

    weight_copy = pltpu.make_async_copy(weight_ref, w_ref, local_sem.at[0])
    weight_copy.start()
    clip_copy = pltpu.make_async_copy(
        clips_ref, clip_pad.at[pl.ds(1, frames), 1], local_sem.at[1]
    )
    clip_copy.start()
    keep_copy = pltpu.make_async_copy(clips_ref, clip_all.at[mine], local_sem.at[2])
    keep_copy.start()

    steps = {(i, t % tm, s) for i in range(dp) for t in (-1, 0, 1) for s in range(rows)}
    steps |= {(0, t, 0) for t in range(tm)}
    steps = sorted(steps - {(0, 0, 0)})
    barrier = pltpu.get_barrier_semaphore()
    for i, t, s in steps:
        pl.semaphore_signal(
            barrier, inc=1, device_id=(shift("dp", i), shift("tm", t), shift("rows", s)),
            device_id_type=MESH,
        )
    for axis, bound, fill in (
        ("rows", 0, lambda pad: pad.at[:, 0]), ("rows", rows - 1, lambda pad: pad.at[:, 2]),
        ("tm", 0, lambda pad: pad.at[0]), ("tm", tm - 1, lambda pad: pad.at[frames + 1]),
    ):
        @pl.when(me[axis] == bound)
        def _():
            for pad in (clip_pad, score_pad, grad_pad):
                at = fill(pad)
                at[...] = jnp.zeros(at.shape, at.dtype)
    for which in range(2):
        for edge in (0, rows + 1):
            shifts[which, :, edge] = jnp.zeros(shifts.shape[1:2] + shifts.shape[3:], shifts.dtype)
        for edge, bound in ((0, 0), (frames + 1, tm - 1)):
            @pl.when(me["tm"] == bound)
            def _():
                slices[which, :, edge] = jnp.zeros((plane, share, cols), slices.dtype)
    pl.semaphore_wait(barrier, len(steps))

    moves = [(t, r) for t in (-1, 0, 1) for r in (-1, 0, 1) if (t, r) != (0, 0)]
    partner = me["rows"] + 1 - 2 * lax.rem(me["rows"], 2) if pair == 2 else me["rows"]
    mirror = rows - 1 - me["rows"]
    toward = partner - me["rows"]

    def inside(t, r):
        ok = None
        for axis, step, size in (("tm", t, tm), ("rows", r, rows)):
            if step:
                cond = me[axis] > 0 if step < 0 else me[axis] < size - 1
                ok = cond if ok is None else jnp.logical_and(ok, cond)
        return ok

    def leaves(t, r, sender):
        ok = inside(t, r) if sender else inside(-t, -r)
        if pair == 1:
            return ok
        row = me["rows"] if sender else me["rows"] - r
        return jnp.logical_and(ok, lax.rem(row, 2) == (0 if r < 0 else 1))

    def halo_copy(which, pad, source, t, r):
        slot = which * len(moves) + moves.index((t, r))
        if t == 0:
            here, there = pl.ds(0, frames), pl.ds(1, frames)
        elif t > 0:
            here, there = pl.ds(frames - 1, 1), pl.ds(0, 1)
        else:
            here, there = pl.ds(0, 1), pl.ds(frames + 1, 1)
        return remote(
            source.at[here], pad.at[there, 1 - r], halo_send.at[slot], halo_recv.at[slot],
            device(tm=me["tm"] + t, rows=me["rows"] + r),
        )

    def hand_copy(which, pad, t):
        at = 2 * which + (t > 0)
        edge = 0 if t > 0 else frames + 1
        return remote(
            pad.at[edge, 1], pad.at[edge, 1 - toward], hand_send.at[at], hand_recv.at[at],
            device(rows=partner),
        )

    def depth_start(which, pad, source):
        for t in (-1, 1):
            @pl.when(inside(t, 0))
            def _():
                halo_copy(which, pad, source, t, 0).start()

    def side_start(which, pad, source):
        for r in (-1, 1):
            @pl.when(inside(0, r))
            def _():
                halo_copy(which, pad, source, 0, r).start()

    def corner_start(which, pad, source):
        for t in (-1, 1):
            for r in (-1, 1):
                @pl.when(leaves(t, r, True))
                def _():
                    halo_copy(which, pad, source, t, r).start()

    def side_sent(which, pad, source):
        for r in (-1, 1):
            @pl.when(inside(0, r))
            def _():
                halo_copy(which, pad, source, 0, r).wait_send()

    def side_wait(which, pad, source):
        for r in (-1, 1):
            @pl.when(inside(0, -r))
            def _():
                halo_copy(which, pad, source, 0, r).wait_recv()

    def depth_wait(which, pad, source):
        for t in (-1, 1):
            @pl.when(inside(-t, 0))
            def _():
                halo_copy(which, pad, source, t, 0).wait_recv()
                if pair == 2:
                    hand_copy(which, pad, t).start()
        for t in (-1, 1):
            @pl.when(inside(t, 0))
            def _():
                halo_copy(which, pad, source, t, 0).wait_send()

    def corner_wait(which, pad, source):
        for t in (-1, 1):
            for r in (-1, 1):
                @pl.when(leaves(t, r, True))
                def _():
                    halo_copy(which, pad, source, t, r).wait_send()

                @pl.when(leaves(t, r, False))
                def _():
                    halo_copy(which, pad, source, t, r).wait_recv()
            if pair == 2:
                @pl.when(inside(-t, 0))
                def _():
                    hand_copy(which, pad, t).wait()

    column = lax.rem(lax.broadcasted_iota(jnp.int32, (count, chans), 0), cols)

    def earlier(value):
        return jnp.where(column == 0, 0.0, pltpu.roll(value, 1, 0))

    def later(value):
        return jnp.where(column == cols - 1, 0.0, pltpu.roll(value, count - 1, 0))

    def conv(which, pad, source, kernel_ref, idle, sent, side, before, between):
        def put(shift_f, start, many, places, new=False):
            if not many:
                return
            left = jnp.concatenate(
                [
                    pad[pl.ds(start + shift_f, many), b].reshape(many * cols, chans)
                    for b in places
                ],
                axis=1,
            )
            at = pl.ds(start * cols, many * cols)
            for d in range(TAPS):
                taps = [kernel_ref[(shift_f * TAPS + b) * TAPS + d] for b in places]
                value = jnp.dot(
                    left, jnp.concatenate(taps, axis=0), preferred_element_type=jnp.float32
                )
                acc[d, at] = value if new else acc[d, at] + value

        def inner_frames(places, new):
            put(1, 0, frames, places, new)
            put(0, 1, frames - 1, places)
            put(2, 0, frames - 1, places)

        def outer_frames(places):
            put(0, 0, 1, places)
            put(2, frames - 1, 1, places)

        inner_frames((1,), True)
        corner_start(which, pad, source)
        idle()
        side(which, pad, source)
        inner_frames((0, 2), False)
        before()
        depth_wait(which, pad, source)
        between()
        outer_frames((1,))
        corner_wait(which, pad, source)
        outer_frames((0, 2))
        sent()
        return earlier(acc[0]) + acc[1] + later(acc[2])

    others = range(1, dp)
    across = [(0, 0)] + [(i, 0) for i in others]
    if near == 2:
        across = [(0, 0), (0, 1)] + [(i, 0) for i in others] + [(i, 1) for i in others]

    edge = jnp.logical_and(me["rows"] > 0, me["rows"] < rows - 1)

    def spot(i, m):
        return shift("dp", -i) * rows + (mirror if m else me["rows"])

    def all_copy(which, buf, i, m):
        at = which * len(across) + across.index((i, m))
        if i == 0:
            block, there = buf.at[mine], device(rows=mirror)
        else:
            block, there = buf.at[spot(0, m)], device(dp=shift("dp", i))
        return remote(block, block, all_send.at[at], all_recv.at[at], there)

    def pass_copy(which, buf, i, m):
        at = which * len(across) + across.index((i, m))
        block = buf.at[spot(i, m)]
        return remote(block, block, pass_send.at[at], pass_recv.at[at], device(rows=partner))

    def all_start(which, buf):
        if pair == 2:
            pass_copy(which, buf, 0, 0).start()
        if near == 2:
            @pl.when(edge)
            def _():
                all_copy(which, buf, 0, 1).start()

    def all_down(which, buf):
        for i in others:
            all_copy(which, buf, i, 0).start()

    def all_side(buf):
        def side(which, pad, source):
            at = which // 2
            if pair == 2:
                pass_copy(at, buf, 0, 0).wait_recv()
                pad[pl.ds(1, frames), 1 + toward] = buf[me["dp"] * rows + partner]
            if near == 2:
                @pl.when(edge)
                def _():
                    all_copy(at, buf, 0, 1).wait_recv()
                    pad[pl.ds(1, frames), 1 - toward] = buf[me["dp"] * rows + mirror]

        return side

    def all_sent(which, buf):
        if near == 2:
            @pl.when(edge)
            def _():
                all_copy(which, buf, 0, 1).wait_send()

    def far_copy(which, buf, i):
        at = which * len(across) + across.index((i, 1))
        block = buf.at[mine]
        return remote(
            block, block, all_send.at[at], all_recv.at[at],
            device(dp=shift("dp", i), rows=mirror),
        )

    def all_between(which, buf):
        if near == 2:
            @pl.when(edge)
            def _():
                for i in others:
                    all_copy(which, buf, i, 1).start()
                pass_copy(which, buf, 0, 1).start()

    def all_outer(which, buf):
        if near == 2:
            @pl.when(jnp.logical_not(edge))
            def _():
                all_copy(which, buf, 0, 1).start()
                for i in others:
                    far_copy(which, buf, i).start()

    def all_relay(which, buf):
        if near == 2:
            @pl.when(jnp.logical_not(edge))
            def _():
                all_copy(which, buf, 0, 1).wait_recv()
                pass_copy(which, buf, 0, 1).start()

    def all_near(which, buf):
        if near == 2:
            pass_copy(which, buf, 0, 1).wait_recv()

    def all_far(which, buf, m):
        if m and near != 2:
            return
        for i in others:
            all_copy(which, buf, i, m).wait_recv()
            if pair == 2:
                pass_copy(which, buf, i, m).start()

    def all_end(which, buf):
        for i, m in across:
            if (i, m) == (0, 1):
                @pl.when(jnp.logical_not(edge))
                def _():
                    all_copy(which, buf, i, m).wait_send()
            elif i:
                all_copy(which, buf, i, m).wait_send()
            if pair == 2:
                pass_copy(which, buf, i, m).wait_send()
                if i:
                    pass_copy(which, buf, i, m).wait_recv()

    def slice_copy(which, t, i, s):
        at = which * 3 + t + 1
        y, r = shift("dp", i), shift("rows", s)
        rest = pl.ds(pl.multiple_of((y * rows + r) * share, share), share)
        if t == 0:
            src, dst = turned.at[which, :, rest], slices.at[which, mine, pl.ds(1, frames)]
        elif t > 0:
            src, dst = turned.at[which, frames - 1, rest], slices.at[which, mine, 0]
        else:
            src, dst = turned.at[which, 0, rest], slices.at[which, mine, frames + 1]
        return remote(
            src, dst, slice_send.at[at], slice_recv.at[at],
            device(dp=y, rows=r, tm=me["tm"] + t),
        )

    pieces = [(i, s) for i in range(dp) for s in range(rows)]

    def slice_start(which, value):
        for f in range(frames):
            turned[which, f] = value[f].T.astype(jnp.bfloat16)
        for t in (1, -1):
            @pl.when(inside(t, 0))
            def _():
                for i, s in pieces:
                    slice_copy(which, t, i, s).start()
        for i, s in pieces[1:]:
            slice_copy(which, 0, i, s).start()
        own = pl.ds(pl.multiple_of(mine * share, share), share)
        for f in range(frames):
            slices[which, mine, f + 1] = turned[which, f, own]

    lane = lax.broadcasted_iota(jnp.int32, (share, cols), 1)

    def slice_end(which):
        def whole(t):
            at = which * 3 + t + 1
            block = slices.at[which, :, 0] if t else slices.at[
                which, pl.ds(0, plane - 1), pl.ds(1, frames)
            ]
            return remote(block, block, slice_send.at[at], slice_recv.at[at], device())

        for t in (1, -1):
            @pl.when(inside(t, 0))
            def _():
                whole(t).wait_send()

            @pl.when(inside(-t, 0))
            def _():
                whole(t).wait_recv()
        whole(0).wait()
        for j in range(plane):
            for f in range(frames + 2):
                value = slices[which, j, f].astype(jnp.float32)
                after = jnp.where(lane == cols - 1, 0.0, pltpu.roll(value, cols - 1, 1))
                before = jnp.where(lane == 0, 0.0, pltpu.roll(value, 1, 1))
                shifts[which, j // rows, j % rows + 1, f] = jnp.concatenate(
                    [after, value, before], axis=0
                ).astype(jnp.bfloat16)

    def correlate(which, buf, a, clips):
        left = jnp.concatenate(
            [
                jnp.concatenate(
                    [
                        shifts[which, y, r + 2 - b, f + 2 - a]
                        for y in clips for r in range(rows) for f in range(frames)
                    ],
                    axis=1,
                )
                for b in range(TAPS)
            ],
            axis=0,
        )
        right = jnp.concatenate(
            [buf[pl.ds(y * rows, rows)].reshape(rows * count, chans) for y in clips], axis=0
        )
        return jnp.dot(left, right, preferred_element_type=jnp.float32)

    def turn_weight():
        def one(k, carry):
            wt_ref[TAPS**3 - 1 - k] = w_ref[k].T
            return carry

        lax.fori_loop(0, TAPS**3, one, 0, unroll=3)

    depth_start(0, clip_pad, clips_ref)
    clip_copy.wait()
    keep_copy.wait()
    all_start(0, clip_all)
    all_down(0, clip_all)
    weight_copy.wait()
    pre = bias_ref[...] + conv(
        0, clip_pad, clips_ref, w_ref, turn_weight, lambda: all_sent(0, clip_all),
        all_side(clip_all), lambda: all_outer(0, clip_all), lambda: all_between(0, clip_all),
    )
    sig = jax.nn.sigmoid(pre)
    slope = sig * (1.0 + pre * (1.0 - sig))
    slope_ref[...] = slope
    curve_ref[...] = sig * (1.0 - sig) * (2.0 + pre * (1.0 - 2.0 * sig))
    score = (head_ref[...] * slope).astype(jnp.bfloat16)
    score_pad[pl.ds(1, frames), 1] = score.reshape(frames, cols, chans)
    score_own = score_pad.at[pl.ds(1, frames), 1]
    depth_start(1, score_pad, score_own)
    side_start(1, score_pad, score_own)
    all_relay(0, clip_all)
    all_far(0, clip_all, 0)

    input_grad = conv(
        1, score_pad, score_own, wt_ref, lambda: None,
        lambda: side_sent(1, score_pad, score_own), side_wait, lambda: None,
        lambda: slice_start(0, score_pad[pl.ds(1, frames), 1].astype(jnp.float32)),
    ).astype(jnp.bfloat16).reshape(frames, cols, chans)
    grad_pad[pl.ds(1, frames), 1] = input_grad
    grad_all[mine] = input_grad
    grad_own = grad_pad.at[pl.ds(1, frames), 1]
    depth_start(2, grad_pad, grad_own)
    all_start(1, grad_all)
    all_down(1, grad_all)
    all_far(0, clip_all, 1)

    back = penalty_weight * conv(
        2, grad_pad, grad_own, w_ref, lambda: None,
        lambda: (all_relay(1, grad_all), all_sent(1, grad_all)),
        all_side(grad_all), lambda: all_outer(1, grad_all), lambda: all_between(1, grad_all),
    )
    pre_grad = back * head_ref[...] * curve_ref[...]
    slice_start(
        1, pre_grad.astype(jnp.bfloat16).astype(jnp.float32).reshape(frames, cols, chans)
    )
    small_mine[...] = jnp.zeros_like(small_mine)
    small_mine[pl.ds(0, 1)] = jnp.sum(pre_grad, axis=0, keepdims=True)
    small_mine[pl.ds(1, 1)] = jnp.sum(back * slope_ref[...], axis=0, keepdims=True)

    def sum_copy(i, s):
        return remote(
            small_mine, small_plane.at[mine], sum_send.at[0], sum_recv.at[0],
            device(dp=shift("dp", i), rows=shift("rows", s)),
        )

    small_plane[mine] = small_mine[...]
    for i, s in pieces[1:]:
        sum_copy(i, s).start()

    slice_end(0)
    all_far(1, grad_all, 0)
    all_near(0, clip_all)
    all_end(0, clip_all)
    all_near(1, grad_all)
    for a in range(TAPS):
        first[a] = correlate(0, grad_all, a, [me["dp"]])
    all_far(1, grad_all, 1)
    all_end(1, grad_all)
    for a in range(TAPS):
        first[a] = penalty_weight * (
            first[a] + correlate(0, grad_all, a, [shift("dp", i) for i in others])
            if dp > 1 else first[a]
        )

    slice_end(1)
    inner, outer = lax.rem(me["tm"], line), me["tm"] // line
    wide = full.shape[-1]
    chunks = [(a, low) for a in range(TAPS) for low in range(chans // wide)]

    def along(step):
        return lax.rem(inner + step, line)

    def part_copy(c, step):
        return remote(
            code.at[c, along(step)], land.at[c, inner], part_send.at[c], part_recv.at[c],
            device(tm=outer * line + along(step)),
        )

    def part_all(c):
        block = land.at[c, pl.ds(0, line - 1)]
        return remote(block, block, part_send.at[c], part_recv.at[c], device())

    def scatter(c):
        a, low = chunks[c]
        if low == 0:
            both = (first[a] + correlate(1, clip_all, a, range(dp))).reshape(taps, share, chans)
            for k in range(chans // wide):
                for t in range(line):
                    total[c + k, t] = both[
                        :, t * part : (t + 1) * part, k * wide : (k + 1) * wide
                    ]
        for step in range(line - 1, 0, -1):
            value, top = encode(total[c, along(step)])
            code[c, along(step), pl.ds(0, taps)] = value
            code[c, along(step), taps] = top
        if c >= 1 and line > 1:
            part_all(c - 1).wait_send()
        for step in range(line - 1, 0, -1):
            part_copy(c, step).start()

    groups = tm // line

    def more_copy(c, step):
        spot = lax.rem(outer + step, groups)
        return remote(
            more.at[c, outer], more.at[c, outer], more_send.at[c], more_recv.at[c],
            device(tm=spot * line + inner),
        )

    upper = inner // 2
    ranks = [inner, inner + 1 - 2 * lax.rem(inner, 2), 2 - upper, 3 - 3 * upper][:line]
    middle = lax.rem(inner + upper, 2) == 1

    def line_copy(c, rank, to):
        here = full.at[c, mine * line + ranks[rank]]
        return remote(
            here, here, line_send.at[c], line_recv.at[c * line + ranks[rank]],
            device(tm=outer * line + to),
        )

    def collect(c):
        value = total[c, inner]
        if line > 1:
            part_all(c).wait_recv()
            if c >= len(chunks) - 1:
                part_all(c).wait_send()
        for step in range(1, line):
            value = value + decode(land[c, along(step)], taps)
        if groups > 1:
            value, top = encode(value)
            more[c, outer, pl.ds(0, taps)] = value
            more[c, outer, taps] = top
            for step in range(1, groups):
                more_copy(c, step).start()
            block = more.at[c, pl.ds(0, groups - 1)]
            remote(block, block, more_send.at[c], more_recv.at[c], device()).wait()
            value = decode(more[c, 0], taps)
            for k in range(1, groups):
                value = value + decode(more[c, k], taps)
        value, top = encode(value)
        full[c, mine * line + inner, pl.ds(0, taps)] = value
        full[c, mine * line + inner, taps] = top
        for rank in range(min(line - 1, 2), 0, -1):
            line_copy(c, 0, ranks[rank]).start()
        share_out(c, 0)

    def share_out(c, rank):
        for side in sides:
            near_copy(c, rank, side).start()
        if pair == 2:
            pair_copy(c, rank, 0).start()

    def take(c, rank):
        if rank > 1:
            @pl.when(jnp.logical_not(middle))
            def _():
                line_copy(c, rank, inner).wait_recv()
        else:
            line_copy(c, rank, inner).wait_recv()
        share_out(c, rank)

    def onward(c):
        if line == 4:
            @pl.when(middle)
            def _():
                for rank in (2, 3):
                    line_copy(c, rank, inner).wait_recv()
                    line_copy(c, rank, ranks[1]).start()

    sides = [("rows", s) for s in range(1, near)] + [("dp", i) for i in range(1, dp)]

    def go(side):
        axis, step = side
        return {axis: shift(axis, step * (pair if axis == "rows" else 1))}

    def come(side):
        axis, step = side
        return {axis: shift(axis, -step * (pair if axis == "rows" else 1))}

    def number(place):
        place = dict(me, **place)
        return place["dp"] * rows + place["rows"]

    turns = [(one, two) for one in sides for two in sides if one[0] != two[0]]
    hops = [()] + [(side,) for side in sides] + turns

    def block_at(c, rank, hop):
        place = {}
        for side in hop:
            place.update(come(side))
        return full.at[c, number(place) * line + ranks[rank]]

    def turned_by(rank):
        return [turn for turn in turns if turn[0][0] == ("dp" if rank % 2 else "rows")]

    per_turn = max(1, len(turns) // 2)

    def near_copy(c, rank, side):
        at = (c * line + rank) * len(sides) + sides.index(side)
        block = block_at(c, rank, ())
        return remote(block, block, near_send.at[c], near_recv.at[at], device(**go(side)))

    def turn_copy(c, rank, turn):
        at = (c * line + rank) * per_turn + turned_by(rank).index(turn)
        block = block_at(c, rank, turn[:1])
        return remote(block, block, turn_send.at[c], turn_recv.at[at], device(**go(turn[1])))

    def pair_copy(c, rank, k):
        block = block_at(c, rank, hops[k])
        return remote(block, block, pair_send.at[c], pair_recv.at[c], device(rows=partner))

    def relay(c, rank):
        for k, side in enumerate(sides):
            near_copy(c, rank, side).wait_recv()
            for turn in turned_by(rank):
                if turn[0] == side:
                    turn_copy(c, rank, turn).start()
            if pair == 2:
                pair_copy(c, rank, 1 + k).start()

    def handover(c, rank):
        for turn in turned_by(rank):
            turn_copy(c, rank, turn).wait_recv()
            if pair == 2:
                pair_copy(c, rank, hops.index(turn)).start()

    def finish(c):
        a, low = chunks[c]
        ended = [(near_send, line * len(sides)), (turn_send, sum(len(turned_by(k)) for k in range(line)))]
        for sem, n in ended + [(line_send, min(line - 1, 2))]:
            if n:
                block = full.at[c, pl.ds(0, n)]
                remote(block, block, sem.at[c], sem.at[c], device()).wait_send()
        if line == 4:
            @pl.when(middle)
            def _():
                block = full.at[c, pl.ds(0, 2)]
                remote(block, block, line_send.at[c], line_send.at[c], device()).wait_send()
        if pair == 2:
            block = full.at[c, pl.ds(0, plane * line // 2)]
            remote(block, block, pair_send.at[c], pair_recv.at[c], device()).wait()
        per = LANES // part

        def tap(k, carry):
            for high in range(chans // LANES):
                for left in range(0, wide, LANES):
                    pile = []
                    for n in range(high * per, (high + 1) * per):
                        block = full.at[c, n]
                        unit = block[taps, :, left : left + LANES].astype(jnp.float32)
                        value = jnp.log(block[k, :, left : left + LANES].astype(jnp.float32))
                        pile.append(value * (unit * (1.0 / (SPAN * math.log(2.0)))))
                    out_ref[
                        a * taps + k, low * wide + left : low * wide + left + LANES,
                        high * LANES : (high + 1) * LANES,
                    ] = jnp.concatenate(pile, axis=0).T
            return carry

        lax.fori_loop(0, taps, tap, 0, unroll=True)

    def end_copy(step):
        return remote(
            small_mine, small_line.at[me["tm"]], end_send.at[0], end_recv.at[0],
            device(tm=shift("tm", step)),
        )

    def small_middle():
        block = small_plane.at[pl.ds(0, plane - 1)]
        if plane > 1:
            remote(block, block, sum_send.at[0], sum_recv.at[0], device()).wait()
        small_mine[...] = jnp.sum(small_plane[...], axis=0)
        small_line[me["tm"]] = small_mine[...]
        for step in range(1, tm):
            end_copy(step).start()

    def small_end():
        block = small_line.at[pl.ds(0, tm - 1)]
        if tm > 1:
            remote(block, block, end_send.at[0], end_recv.at[0], device()).wait()
        value = jnp.sum(small_line[...], axis=0)
        bias_out[...] = value[0:1]
        head_out[...] = value[1:2]

    pace = 2.65 * wide / LANES
    order = [(4.0, small_middle, ()), (16.0, small_end, ())]
    for c in range(len(chunks)):
        got = 4.9 + pace * c
        order += [
            (got - 5.2 , scatter, (c,)), (got, collect, (c,)), (got + 4.5, onward, (c,)),
            (got + 19.0, finish, (c,)),
        ]
        for rank in range(line):
            if rank:
                order.append((got + (0, 4.4, 8.5, 8.5)[rank], take, (c, rank)))
            order += [
                (got + (4.6, 8.6, 12.5, 12.5)[rank], relay, (c, rank)), (got + (8.7, 12.6, 16.5, 16.5)[rank], handover, (c, rank)),
            ]
    for _, stage, what in sorted(order, key=lambda entry: entry[0]):
        stage(*what)


def put_out(grad_ref, bias_ref, head_ref, grad_out, bias_out, head_out, sem):
    taps = TAPS**2
    copies = [
        pltpu.make_async_copy(
            grad_ref.at[pl.ds(k * TAPS, TAPS)], grad_out.at[pl.ds(k * TAPS, TAPS)], sem.at[k]
        )
        for k in range(taps)
    ]
    copies.append(pltpu.make_async_copy(bias_ref, bias_out, sem.at[taps]))
    copies.append(pltpu.make_async_copy(head_ref, head_out, sem.at[taps + 1]))
    for copy in copies:
        copy.start()
    for copy in copies:
        copy.wait()


def per_device(sizes, clips, weight, bias, head):
    dp, tm, rows = sizes
    _, frames, _, cols, chans = clips.shape
    count = frames * cols
    plane = dp * rows
    share = chans // plane
    line, groups = split_line(tm, share // SUB)
    part = share // line
    taps = TAPS**2
    pair = 2 if rows % 2 == 0 else 1
    near = rows // pair
    if rows not in (1, 2, 4):
        raise ValueError("rows")
    sides = near - 1 + dp - 1
    turns = 2 * (near - 1) * (dp - 1)
    pad = pltpu.VMEM((frames + 2, 3, cols, chans), jnp.bfloat16)
    field = pltpu.VMEM((count, chans), jnp.float32)
    gathered = pltpu.VMEM((plane, frames, cols, chans), jnp.bfloat16)
    wide = WIDE if chans % WIDE == 0 else chans
    chunks = TAPS * (chans // wide)
    coded = pltpu.VMEM((chunks, line, taps + 1, part, wide), jnp.bfloat16)

    def dma(n):
        return pltpu.SemaphoreType.DMA((max(n, 1),))

    sems = []
    for send, recv in (
        (24, 24), (6, 6), (2 * dp * near, 2 * dp * near), (2 * dp * near, 2 * dp * near),
        (6, 6), (chunks, chunks),
        (chunks, chunks) if groups > 1 else (1, 1), (chunks, chunks * line),
        (chunks, chunks * line * sides), (chunks, chunks * line * max(1, turns // 2)),
        (chunks, chunks), (1, 1), (1, 1),
    ):
        sems += [dma(send), dma(recv)]
    vmem = pl.BlockSpec(memory_space=pltpu.VMEM)
    hbm = pl.BlockSpec(memory_space=pl.ANY)
    grad_weight, grad_bias, grad_head = pl.pallas_call(
        functools.partial(kernel, sizes, line),
        out_shape=(
            pltpu.VMEM((TAPS**3, chans, chans), jnp.float32),
            pltpu.VMEM((1, chans), jnp.float32),
            pltpu.VMEM((1, chans), jnp.float32),
        ),
        in_specs=[hbm, hbm, vmem, vmem],
        out_specs=(vmem, vmem, vmem),
        scratch_shapes=[
            pltpu.VMEM((TAPS**3, chans, chans), jnp.bfloat16),
            pltpu.VMEM((TAPS**3, chans, chans), jnp.bfloat16),
            pad, pad, pad,
            pltpu.VMEM((TAPS, count, chans), jnp.float32),
            field, field,
            gathered, gathered,
            pltpu.VMEM((2, frames, chans, cols), jnp.bfloat16),
            pltpu.VMEM((2, plane, frames + 2, share, cols), jnp.bfloat16),
            pltpu.VMEM((2, dp, rows + 2, frames + 2, TAPS * share, cols), jnp.bfloat16),
            pltpu.VMEM((TAPS, taps * share, chans), jnp.float32),
            pltpu.VMEM((chunks, line, taps, part, wide), jnp.float32),
            coded, coded,
            pltpu.VMEM((chunks, groups, taps + 1, part, wide), jnp.bfloat16),
            pltpu.VMEM((chunks, plane * line, taps + 1, part, wide), jnp.bfloat16),
            pltpu.VMEM((SUB, chans), jnp.float32),
            pltpu.VMEM((plane, SUB, chans), jnp.float32),
            pltpu.VMEM((tm, SUB, chans), jnp.float32),
            dma(3), *sems,
        ],
        compiler_params=pltpu.CompilerParams(
            collective_id=0, has_side_effects=True, vmem_limit_bytes=48 * 1024 * 1024
        ),
    )(
        pltpu.with_memory_space_constraint(clips.reshape(frames, cols, chans), pltpu.HBM),
        weight.reshape(TAPS**3, chans, chans),
        bias.reshape(1, chans),
        head.reshape(1, chans),
    )
    row = jax.ShapeDtypeStruct((1, chans), jnp.float32)
    grad_weight, grad_bias, grad_head = pl.pallas_call(
        put_out,
        out_shape=(jax.ShapeDtypeStruct((TAPS**3, chans, chans), jnp.float32), row, row),
        in_specs=[vmem, vmem, vmem],
        out_specs=(hbm, hbm, hbm),
        scratch_shapes=[pltpu.SemaphoreType.DMA((TAPS**2 + 2,))],
        compiler_params=pltpu.CompilerParams(vmem_limit_bytes=8 * 1024 * 1024),
    )(grad_weight, grad_bias, grad_head)
    grad_weight = grad_weight.reshape(TAPS, TAPS, TAPS, chans, chans)
    return grad_weight, grad_bias.reshape(chans), grad_head.reshape(chans)


def solution(mesh):
    sizes = tuple(mesh.shape[axis] for axis in ("dp", "tm", "rows"))
    return jax.shard_map(
        functools.partial(per_device, sizes),
        mesh=mesh,
        in_specs=(P("dp", "tm", "rows", None, None), P(), P(), P()),
        out_specs=(P(), P(), P()),
        check_vma=False,
    )
```

```python
import functools
import math

import jax
import jax.numpy as jnp
from jax import lax
from jax.experimental import pallas as pl
from jax.experimental.pallas import tpu as pltpu
from jax.sharding import PartitionSpec as P

penalty_weight = 0.01
MESH = pl.DeviceIdType.MESH
SUB = 8
TAPS = 3
SPAN = 120.0
LANES = 128
WIDE = 128


def split_line(tm, most):
    line = 1
    while tm % (2 * line) == 0 and 2 * line <= most:
        line *= 2
    return line, tm // line


def decode(block, taps):
    unit = block[taps].astype(jnp.float32) * (1.0 / (SPAN * math.log(2.0)))
    return jnp.log(block[:taps].astype(jnp.float32)) * unit[None]


def encode(value):
    top = (jnp.max(jnp.abs(value), axis=0) * 1.01 + 1e-30).astype(jnp.bfloat16)
    rate = SPAN / top.astype(jnp.float32)
    return jnp.exp2(value * rate[None]).astype(jnp.bfloat16), top


def kernel(
    sizes, line, clips_ref, weight_ref, bias_ref, head_ref,
    out_ref, bias_out, head_out,
    w_ref, wt_ref, clip_pad, score_pad, grad_pad, acc, slope_ref, curve_ref,
    clip_all, grad_all, turned, slices, shifts, first, total, code, land, more, full,
    small_mine, small_plane, small_line,
    local_sem, halo_send, halo_recv, hand_send, hand_recv, all_send, all_recv, pass_send, pass_recv,
    slice_send, slice_recv, part_send, part_recv, more_send, more_recv,
    line_send, line_recv, near_send, near_recv, turn_send, turn_recv, pair_send, pair_recv,
    sum_send, sum_recv, end_send, end_recv,
):
    dp, tm, rows = sizes
    frames, cols, chans = clips_ref.shape
    count = frames * cols
    plane = dp * rows
    share = chans // plane
    part = share // line
    taps = TAPS**2
    pair = 2 if rows % 2 == 0 else 1
    near = rows // pair
    me = {"dp": lax.axis_index("dp"), "tm": lax.axis_index("tm"), "rows": lax.axis_index("rows")}
    mine = me["dp"] * rows + me["rows"]

    def device(**moved):
        place = dict(me, **moved)
        return (place["dp"], place["tm"], place["rows"])

    def shift(axis, step):
        return lax.rem(me[axis] + step % dict(dp=dp, tm=tm, rows=rows)[axis], dict(dp=dp, tm=tm, rows=rows)[axis])

    def remote(src, dst, send, recv, target):
        return pltpu.make_async_remote_copy(
            src_ref=src, dst_ref=dst, send_sem=send, recv_sem=recv,
            device_id=target, device_id_type=MESH,
        )

    weight_copy = pltpu.make_async_copy(weight_ref, w_ref, local_sem.at[0])
    weight_copy.start()
    clip_copy = pltpu.make_async_copy(
        clips_ref, clip_pad.at[pl.ds(1, frames), 1], local_sem.at[1]
    )
    clip_copy.start()
    keep_copy = pltpu.make_async_copy(clips_ref, clip_all.at[mine], local_sem.at[2])
    keep_copy.start()

    steps = {(i, t % tm, s) for i in range(dp) for t in (-1, 0, 1) for s in range(rows)}
    steps |= {(0, t, 0) for t in range(tm)}
    steps = sorted(steps - {(0, 0, 0)})
    barrier = pltpu.get_barrier_semaphore()
    for i, t, s in steps:
        pl.semaphore_signal(
            barrier, inc=1, device_id=(shift("dp", i), shift("tm", t), shift("rows", s)),
            device_id_type=MESH,
        )
    def clear(pads):
        for axis, bound, fill in (
            ("rows", 0, lambda pad: pad.at[:, 0]), ("rows", rows - 1, lambda pad: pad.at[:, 2]),
            ("tm", 0, lambda pad: pad.at[0]), ("tm", tm - 1, lambda pad: pad.at[frames + 1]),
        ):
            @pl.when(me[axis] == bound)
            def _():
                for pad in pads:
                    at = fill(pad)
                    at[...] = jnp.zeros(at.shape, at.dtype)

    def clear_later():
        clear((score_pad, grad_pad))
        for which in range(2):
            for rim in (0, rows + 1):
                shifts[which, :, rim] = jnp.zeros(
                    shifts.shape[1:2] + shifts.shape[3:], shifts.dtype
                )
            for rim, bound in ((0, 0), (frames + 1, tm - 1)):
                @pl.when(me["tm"] == bound)
                def _():
                    slices[which, :, rim] = jnp.zeros((plane, share, cols), slices.dtype)

    clear((clip_pad,))
    pl.semaphore_wait(barrier, len(steps))

    moves = [(t, r) for t in (-1, 0, 1) for r in (-1, 0, 1) if (t, r) != (0, 0)]
    partner = me["rows"] + 1 - 2 * lax.rem(me["rows"], 2) if pair == 2 else me["rows"]
    mirror = rows - 1 - me["rows"]
    toward = partner - me["rows"]

    def inside(t, r):
        ok = None
        for axis, step, size in (("tm", t, tm), ("rows", r, rows)):
            if step:
                cond = me[axis] > 0 if step < 0 else me[axis] < size - 1
                ok = cond if ok is None else jnp.logical_and(ok, cond)
        return ok

    def leaves(t, r, sender):
        ok = inside(t, r) if sender else inside(-t, -r)
        if pair == 1:
            return ok
        row = me["rows"] if sender else me["rows"] - r
        return jnp.logical_and(ok, lax.rem(row, 2) == (0 if r < 0 else 1))

    def halo_copy(which, pad, source, t, r):
        slot = which * len(moves) + moves.index((t, r))
        if t == 0:
            here, there = pl.ds(0, frames), pl.ds(1, frames)
        elif t > 0:
            here, there = pl.ds(frames - 1, 1), pl.ds(0, 1)
        else:
            here, there = pl.ds(0, 1), pl.ds(frames + 1, 1)
        return remote(
            source.at[here], pad.at[there, 1 - r], halo_send.at[slot], halo_recv.at[slot],
            device(tm=me["tm"] + t, rows=me["rows"] + r),
        )

    def hand_copy(which, pad, t):
        at = 2 * which + (t > 0)
        edge = 0 if t > 0 else frames + 1
        return remote(
            pad.at[edge, 1], pad.at[edge, 1 - toward], hand_send.at[at], hand_recv.at[at],
            device(rows=partner),
        )

    def depth_start(which, pad, source):
        for t in (-1, 1):
            @pl.when(inside(t, 0))
            def _():
                halo_copy(which, pad, source, t, 0).start()

    def side_start(which, pad, source):
        for r in (-1, 1):
            @pl.when(inside(0, r))
            def _():
                halo_copy(which, pad, source, 0, r).start()

    def corner_start(which, pad, source):
        for t in (-1, 1):
            for r in (-1, 1):
                @pl.when(leaves(t, r, True))
                def _():
                    halo_copy(which, pad, source, t, r).start()

    def side_sent(which, pad, source):
        for r in (-1, 1):
            @pl.when(inside(0, r))
            def _():
                halo_copy(which, pad, source, 0, r).wait_send()

    def side_wait(which, pad, source, close):
        for r in (-1, 1):
            here = leaves(0, r, False)
            if close:
                here = jnp.logical_and(inside(0, -r), jnp.logical_not(here))

            @pl.when(here)
            def _():
                halo_copy(which, pad, source, 0, r).wait_recv()

    def depth_wait(which, pad, source):
        for t in (-1, 1):
            @pl.when(inside(-t, 0))
            def _():
                halo_copy(which, pad, source, t, 0).wait_recv()
                if pair == 2:
                    hand_copy(which, pad, t).start()
        for t in (-1, 1):
            @pl.when(inside(t, 0))
            def _():
                halo_copy(which, pad, source, t, 0).wait_send()

    def corner_wait(which, pad, source):
        for t in (-1, 1):
            for r in (-1, 1):
                @pl.when(leaves(t, r, True))
                def _():
                    halo_copy(which, pad, source, t, r).wait_send()

                @pl.when(leaves(t, r, False))
                def _():
                    halo_copy(which, pad, source, t, r).wait_recv()

    def hand_wait(which, pad):
        for t in (-1, 1):
            if pair == 2:
                @pl.when(inside(-t, 0))
                def _():
                    hand_copy(which, pad, t).wait()

    column = lax.rem(lax.broadcasted_iota(jnp.int32, (count, chans), 0), cols)

    def earlier(value):
        return jnp.where(column == 0, 0.0, pltpu.roll(value, 1, 0))

    def later(value):
        return jnp.where(column == cols - 1, 0.0, pltpu.roll(value, count - 1, 0))

    def conv(which, pad, source, kernel_ref, idle, sent, side, before, after, between):
        def put(shift_f, start, many, places, new=False):
            if not many or not places:
                return
            left = jnp.concatenate(
                [
                    pad[pl.ds(start + shift_f, many), b].reshape(many * cols, chans)
                    for b in places
                ],
                axis=1,
            )
            at = pl.ds(start * cols, many * cols)
            for d in range(TAPS):
                taps = [kernel_ref[(shift_f * TAPS + b) * TAPS + d] for b in places]
                value = jnp.dot(
                    left, jnp.concatenate(taps, axis=0), preferred_element_type=jnp.float32
                )
                acc[d, at] = value if new else acc[d, at] + value

        def inner_frames(places, new):
            put(1, 0, frames, places, new)
            put(0, 1, frames - 1, places)
            put(2, 0, frames - 1, places)

        def outer_frames(places):
            put(0, 0, 1, places)
            put(2, frames - 1, 1, places)

        close, far = ((1 + toward,), (1 - toward,)) if pair == 2 else ((), (0, 2))
        inner_frames((1,), True)
        corner_start(which, pad, source)
        idle()
        side(which, pad, source, True)
        inner_frames(close, False)
        before()
        depth_wait(which, pad, source)
        outer_frames((1,))
        hand_wait(which, pad)
        outer_frames(close)
        after()
        side(which, pad, source, False)
        between()
        inner_frames(far, False)
        corner_wait(which, pad, source)
        outer_frames(far)
        sent()
        return earlier(acc[0]) + acc[1] + later(acc[2])

    others = range(1, dp)
    across = [(0, 0)] + [(i, 0) for i in others]
    if near == 2:
        across = [(0, 0), (0, 1)] + [(i, 0) for i in others] + [(i, 1) for i in others]

    edge = jnp.logical_and(me["rows"] > 0, me["rows"] < rows - 1)

    def spot(i, m):
        return shift("dp", -i) * rows + (mirror if m else me["rows"])

    def all_copy(which, buf, i, m):
        at = which * len(across) + across.index((i, m))
        if i == 0:
            block, there = buf.at[mine], device(rows=mirror)
        else:
            block, there = buf.at[spot(0, m)], device(dp=shift("dp", i))
        return remote(block, block, all_send.at[at], all_recv.at[at], there)

    def pass_copy(which, buf, i, m):
        at = which * len(across) + across.index((i, m))
        block = buf.at[spot(i, m)]
        return remote(block, block, pass_send.at[at], pass_recv.at[at], device(rows=partner))

    def all_start(which, buf):
        if pair == 2:
            pass_copy(which, buf, 0, 0).start()
        if near == 2:
            @pl.when(edge)
            def _():
                all_copy(which, buf, 0, 1).start()

    def all_down(which, buf):
        for i in others:
            all_copy(which, buf, i, 0).start()

    def all_side(buf):
        def side(which, pad, source, close):
            at = which // 2
            if pair == 2 and close:
                pass_copy(at, buf, 0, 0).wait_recv()
                pad[pl.ds(1, frames), 1 + toward] = buf[me["dp"] * rows + partner]
            if near == 2 and not close:
                @pl.when(edge)
                def _():
                    all_copy(at, buf, 0, 1).wait_recv()
                    pad[pl.ds(1, frames), 1 - toward] = buf[me["dp"] * rows + mirror]

        return side

    def all_sent(which, buf):
        if near == 2:
            @pl.when(edge)
            def _():
                all_copy(which, buf, 0, 1).wait_send()

    def far_copy(which, buf, i):
        at = which * len(across) + across.index((i, 1))
        block = buf.at[mine]
        return remote(
            block, block, all_send.at[at], all_recv.at[at],
            device(dp=shift("dp", i), rows=mirror),
        )

    def all_between(which, buf):
        if near == 2:
            @pl.when(edge)
            def _():
                for i in others:
                    all_copy(which, buf, i, 1).start()
                pass_copy(which, buf, 0, 1).start()

    def all_outer(which, buf):
        if near == 2:
            @pl.when(jnp.logical_not(edge))
            def _():
                all_copy(which, buf, 0, 1).start()
                for i in others:
                    far_copy(which, buf, i).start()

    def all_relay(which, buf):
        if near == 2:
            @pl.when(jnp.logical_not(edge))
            def _():
                all_copy(which, buf, 0, 1).wait_recv()
                pass_copy(which, buf, 0, 1).start()

    def all_near(which, buf):
        if near == 2:
            pass_copy(which, buf, 0, 1).wait_recv()

    def all_far(which, buf, m):
        if m and near != 2:
            return
        for i in others:
            all_copy(which, buf, i, m).wait_recv()
            if pair == 2:
                pass_copy(which, buf, i, m).start()

    def all_end(which, buf):
        for i, m in across:
            if (i, m) == (0, 1):
                @pl.when(jnp.logical_not(edge))
                def _():
                    all_copy(which, buf, i, m).wait_send()
            elif i:
                all_copy(which, buf, i, m).wait_send()
            if pair == 2:
                pass_copy(which, buf, i, m).wait_send()
                if i:
                    pass_copy(which, buf, i, m).wait_recv()

    def slice_copy(which, t, i, s):
        at = which * 3 + t + 1
        y, r = shift("dp", i), shift("rows", s)
        rest = pl.ds(pl.multiple_of((y * rows + r) * share, share), share)
        if t == 0:
            src, dst = turned.at[which, :, rest], slices.at[which, mine, pl.ds(1, frames)]
        elif t > 0:
            src, dst = turned.at[which, frames - 1, rest], slices.at[which, mine, 0]
        else:
            src, dst = turned.at[which, 0, rest], slices.at[which, mine, frames + 1]
        return remote(
            src, dst, slice_send.at[at], slice_recv.at[at],
            device(dp=y, rows=r, tm=me["tm"] + t),
        )

    pieces = [(i, s) for i in range(dp) for s in range(rows)]

    def slice_turn(which, value):
        for f in range(frames):
            turned[which, f] = value[f].T

    def slice_start(which):
        for t in (1, -1):
            @pl.when(inside(t, 0))
            def _():
                for i, s in pieces:
                    slice_copy(which, t, i, s).start()
        for i, s in pieces[1:]:
            slice_copy(which, 0, i, s).start()
        own = pl.ds(pl.multiple_of(mine * share, share), share)
        for f in range(frames):
            slices[which, mine, f + 1] = turned[which, f, own]

    lane = lax.broadcasted_iota(jnp.int32, (share, cols), 1)

    def slice_end(which):
        def whole(t):
            at = which * 3 + t + 1
            block = slices.at[which, :, 0] if t else slices.at[
                which, pl.ds(0, plane - 1), pl.ds(1, frames)
            ]
            return remote(block, block, slice_send.at[at], slice_recv.at[at], device())

        for t in (1, -1):
            @pl.when(inside(t, 0))
            def _():
                whole(t).wait_send()

            @pl.when(inside(-t, 0))
            def _():
                whole(t).wait_recv()
        whole(0).wait()
        for j in range(plane):
            for f in range(frames + 2):
                value = slices[which, j, f].astype(jnp.float32)
                after = jnp.where(lane == cols - 1, 0.0, pltpu.roll(value, cols - 1, 1))
                before = jnp.where(lane == 0, 0.0, pltpu.roll(value, 1, 1))
                shifts[which, j // rows, j % rows + 1, f] = jnp.concatenate(
                    [after, value, before], axis=0
                ).astype(jnp.bfloat16)

    def correlate(which, buf, a, clips):
        left = jnp.concatenate(
            [
                jnp.concatenate(
                    [
                        shifts[which, y, r + 2 - b, f + 2 - a]
                        for y in clips for r in range(rows) for f in range(frames)
                    ],
                    axis=1,
                )
                for b in range(TAPS)
            ],
            axis=0,
        )
        right = jnp.concatenate(
            [buf[pl.ds(y * rows, rows)].reshape(rows * count, chans) for y in clips], axis=0
        )
        return jnp.dot(left, right, preferred_element_type=jnp.float32)

    def turn_weight():
        def one(k, carry):
            wt_ref[TAPS**3 - 1 - k] = w_ref[k].T
            return carry

        lax.fori_loop(0, TAPS**3, one, 0, unroll=3)
        clear_later()

    depth_start(0, clip_pad, clips_ref)
    clip_copy.wait()
    keep_copy.wait()
    all_start(0, clip_all)
    all_down(0, clip_all)
    weight_copy.wait()
    pre = bias_ref[...] + conv(
        0, clip_pad, clips_ref, w_ref, turn_weight, lambda: all_sent(0, clip_all),
        all_side(clip_all), lambda: all_outer(0, clip_all), lambda: None,
        lambda: all_between(0, clip_all),
    )
    sig = jax.nn.sigmoid(pre)
    slope = sig * (1.0 + pre * (1.0 - sig))
    slope_ref[...] = slope
    curve_ref[...] = sig * (1.0 - sig) * (2.0 + pre * (1.0 - 2.0 * sig))
    score = (head_ref[...] * slope).astype(jnp.bfloat16)
    score_pad[pl.ds(1, frames), 1] = score.reshape(frames, cols, chans)
    score_own = score_pad.at[pl.ds(1, frames), 1]
    depth_start(1, score_pad, score_own)
    side_start(1, score_pad, score_own)
    all_relay(0, clip_all)
    all_far(0, clip_all, 0)

    input_grad = conv(
        1, score_pad, score_own, wt_ref, lambda: None,
        lambda: side_sent(1, score_pad, score_own), side_wait, lambda: None,
        lambda: slice_turn(0, score_pad[pl.ds(1, frames), 1]),
        lambda: slice_start(0),
    ).astype(jnp.bfloat16).reshape(frames, cols, chans)
    grad_pad[pl.ds(1, frames), 1] = input_grad
    grad_all[mine] = input_grad
    grad_own = grad_pad.at[pl.ds(1, frames), 1]
    depth_start(2, grad_pad, grad_own)
    all_start(1, grad_all)
    all_down(1, grad_all)
    all_far(0, clip_all, 1)

    back = penalty_weight * conv(
        2, grad_pad, grad_own, w_ref, lambda: None,
        lambda: (all_relay(1, grad_all), all_sent(1, grad_all)),
        all_side(grad_all), lambda: all_outer(1, grad_all), lambda: None,
        lambda: all_between(1, grad_all),
    )
    pre_grad = back * head_ref[...] * curve_ref[...]
    slice_turn(
        1, pre_grad.astype(jnp.bfloat16).reshape(frames, cols, chans)
    )
    slice_start(1)
    small_mine[...] = jnp.zeros_like(small_mine)
    small_mine[pl.ds(0, 1)] = jnp.sum(pre_grad, axis=0, keepdims=True)
    small_mine[pl.ds(1, 1)] = jnp.sum(back * slope_ref[...], axis=0, keepdims=True)

    def sum_copy(i, s):
        return remote(
            small_mine, small_plane.at[mine], sum_send.at[0], sum_recv.at[0],
            device(dp=shift("dp", i), rows=shift("rows", s)),
        )

    small_plane[mine] = small_mine[...]
    for i, s in pieces[1:]:
        sum_copy(i, s).start()

    slice_end(0)
    all_far(1, grad_all, 0)
    all_near(0, clip_all)
    all_end(0, clip_all)
    all_near(1, grad_all)
    for a in range(TAPS):
        first[a] = correlate(0, grad_all, a, [me["dp"]])
    all_far(1, grad_all, 1)
    slice_end(1)
    for a in range(TAPS):
        first[a] = penalty_weight * first[a] + correlate(1, clip_all, a, range(dp))
    all_end(1, grad_all)
    inner, outer = lax.rem(me["tm"], line), me["tm"] // line
    wide = full.shape[-1]
    chunks = [(a, low) for a in range(TAPS) for low in range(chans // wide)]

    def along(step):
        return lax.rem(inner + step, line)

    def part_copy(c, step):
        return remote(
            code.at[c, along(step)], land.at[c, inner], part_send.at[c], part_recv.at[c],
            device(tm=outer * line + along(step)),
        )

    def part_all(c):
        block = land.at[c, pl.ds(0, line - 1)]
        return remote(block, block, part_send.at[c], part_recv.at[c], device())

    def product(a):
        both = first[a]
        if dp > 1:
            both = both + penalty_weight * correlate(
                0, grad_all, a, [shift("dp", i) for i in others]
            )
        both = both.reshape(taps, share, chans)
        for k in range(chans // wide):
            for t in range(line):
                total[a * (chans // wide) + k, t] = both[
                    :, t * part : (t + 1) * part, k * wide : (k + 1) * wide
                ]

    def scatter(c):
        for step in range(line - 1, 0, -1):
            value, top = encode(total[c, along(step)])
            code[c, along(step), pl.ds(0, taps)] = value
            code[c, along(step), taps] = top
        if c >= 1 and line > 1:
            part_all(c - 1).wait_send()
        for step in range(line - 1, 0, -1):
            part_copy(c, step).start()

    groups = tm // line

    def more_copy(c, step):
        spot = lax.rem(outer + step, groups)
        return remote(
            more.at[c, outer], more.at[c, outer], more_send.at[c], more_recv.at[c],
            device(tm=spot * line + inner),
        )

    upper = inner // 2
    ranks = [inner, inner + 1 - 2 * lax.rem(inner, 2), 2 - upper, 3 - 3 * upper][:line]
    middle = lax.rem(inner + upper, 2) == 1

    def line_copy(c, rank, to):
        here = full.at[c, mine * line + ranks[rank]]
        return remote(
            here, here, line_send.at[c], line_recv.at[c * line + ranks[rank]],
            device(tm=outer * line + to),
        )

    def collect(c):
        value = total[c, inner]
        if line > 1:
            part_all(c).wait_recv()
            if c >= len(chunks) - 1:
                part_all(c).wait_send()
        for step in range(1, line):
            value = value + decode(land[c, along(step)], taps)
        if groups > 1:
            value, top = encode(value)
            more[c, outer, pl.ds(0, taps)] = value
            more[c, outer, taps] = top
            for step in range(1, groups):
                more_copy(c, step).start()
            block = more.at[c, pl.ds(0, groups - 1)]
            remote(block, block, more_send.at[c], more_recv.at[c], device()).wait()
            value = decode(more[c, 0], taps)
            for k in range(1, groups):
                value = value + decode(more[c, k], taps)
        value, top = encode(value)
        full[c, mine * line + inner, pl.ds(0, taps)] = value
        full[c, mine * line + inner, taps] = top
        for rank in range(min(line - 1, 2), 0, -1):
            line_copy(c, 0, ranks[rank]).start()
        share_out(c, 0)

    def share_out(c, rank):
        for side in sides:
            near_copy(c, rank, side).start()
        if pair == 2:
            pair_copy(c, rank, 0).start()

    def take(c, rank):
        if rank > 1:
            @pl.when(jnp.logical_not(middle))
            def _():
                line_copy(c, rank, inner).wait_recv()
        else:
            line_copy(c, rank, inner).wait_recv()
        share_out(c, rank)

    def onward(c):
        if line == 4:
            @pl.when(middle)
            def _():
                for rank in (2, 3):
                    line_copy(c, rank, inner).wait_recv()
                    line_copy(c, rank, ranks[1]).start()

    sides = [("rows", s) for s in range(1, near)] + [("dp", i) for i in range(1, dp)]

    def go(side):
        axis, step = side
        return {axis: shift(axis, step * (pair if axis == "rows" else 1))}

    def come(side):
        axis, step = side
        return {axis: shift(axis, -step * (pair if axis == "rows" else 1))}

    def number(place):
        place = dict(me, **place)
        return place["dp"] * rows + place["rows"]

    turns = [(one, two) for one in sides for two in sides if one[0] != two[0]]
    hops = [()] + [(side,) for side in sides] + turns

    def block_at(c, rank, hop):
        place = {}
        for side in hop:
            place.update(come(side))
        return full.at[c, number(place) * line + ranks[rank]]

    def turned_by(rank):
        return [turn for turn in turns if turn[0][0] == ("dp" if rank % 2 else "rows")]

    per_turn = max(1, len(turns) // 2)

    def near_copy(c, rank, side):
        at = (c * line + rank) * len(sides) + sides.index(side)
        block = block_at(c, rank, ())
        return remote(block, block, near_send.at[c], near_recv.at[at], device(**go(side)))

    def turn_copy(c, rank, turn):
        at = (c * line + rank) * per_turn + turned_by(rank).index(turn)
        block = block_at(c, rank, turn[:1])
        return remote(block, block, turn_send.at[c], turn_recv.at[at], device(**go(turn[1])))

    def pair_copy(c, rank, k):
        block = block_at(c, rank, hops[k])
        return remote(block, block, pair_send.at[c], pair_recv.at[c], device(rows=partner))

    def relay(c, rank):
        for k, side in enumerate(sides):
            near_copy(c, rank, side).wait_recv()
            for turn in turned_by(rank):
                if turn[0] == side:
                    turn_copy(c, rank, turn).start()
            if pair == 2:
                pair_copy(c, rank, 1 + k).start()

    def handover(c, rank):
        for turn in turned_by(rank):
            turn_copy(c, rank, turn).wait_recv()
            if pair == 2:
                pair_copy(c, rank, hops.index(turn)).start()

    def finish(c):
        a, low = chunks[c]
        ended = [(near_send, line * len(sides)), (turn_send, sum(len(turned_by(k)) for k in range(line)))]
        for sem, n in ended + [(line_send, min(line - 1, 2))]:
            if n:
                block = full.at[c, pl.ds(0, n)]
                remote(block, block, sem.at[c], sem.at[c], device()).wait_send()
        if line == 4:
            @pl.when(middle)
            def _():
                block = full.at[c, pl.ds(0, 2)]
                remote(block, block, line_send.at[c], line_send.at[c], device()).wait_send()
        if pair == 2:
            block = full.at[c, pl.ds(0, plane * line // 2)]
            remote(block, block, pair_send.at[c], pair_recv.at[c], device()).wait()
        per = LANES // part

        def tap(k, carry):
            for high in range(chans // LANES):
                for left in range(0, wide, LANES):
                    pile = []
                    for n in range(high * per, (high + 1) * per):
                        block = full.at[c, n]
                        unit = block[taps, :, left : left + LANES].astype(jnp.float32)
                        value = jnp.log(block[k, :, left : left + LANES].astype(jnp.float32))
                        pile.append(value * (unit * (1.0 / (SPAN * math.log(2.0)))))
                    out_ref[
                        a * taps + k, low * wide + left : low * wide + left + LANES,
                        high * LANES : (high + 1) * LANES,
                    ] = jnp.concatenate(pile, axis=0).T
            return carry

        lax.fori_loop(0, taps, tap, 0, unroll=True)

    def end_copy(step):
        return remote(
            small_mine, small_line.at[me["tm"]], end_send.at[0], end_recv.at[0],
            device(tm=shift("tm", step)),
        )

    def small_middle():
        block = small_plane.at[pl.ds(0, plane - 1)]
        if plane > 1:
            remote(block, block, sum_send.at[0], sum_recv.at[0], device()).wait()
        small_mine[...] = jnp.sum(small_plane[...], axis=0)
        small_line[me["tm"]] = small_mine[...]
        for step in range(1, tm):
            end_copy(step).start()

    def small_end():
        block = small_line.at[pl.ds(0, tm - 1)]
        if tm > 1:
            remote(block, block, end_send.at[0], end_recv.at[0], device()).wait()
        value = jnp.sum(small_line[...], axis=0)
        bias_out[...] = value[0:1]
        head_out[...] = value[1:2]

    pace = 2.65 * wide / LANES
    order = [(4.0, small_middle, ()), (16.0, small_end, ()), (-9.0, product, (0,))]
    order += [(got_a, product, (a,)) for a, got_a in ((1, 0.1), (2, 2.0))]
    for c in range(len(chunks)):
        got = 4.9 + pace * c
        order += [
            (got - 5.2, scatter, (c,)), (got, collect, (c,)), (got + 2.8, onward, (c,)),
            (got + 23.0, finish, (c,)),
        ]
        for rank in range(line):
            if rank:
                order.append((got + (0, 2.9, 5.4, 5.5)[rank], take, (c, rank)))
            order += [
                (got + (7.0, 10.0, 13.0, 13.1)[rank], relay, (c, rank)),
                (got + (13.2, 16.0, 19.0, 19.1)[rank], handover, (c, rank)),
            ]
    for _, stage, what in sorted(order, key=lambda entry: entry[0]):
        stage(*what)


def put_out(grad_ref, bias_ref, head_ref, grad_out, bias_out, head_out, sem):
    taps = TAPS**2
    copies = [
        pltpu.make_async_copy(
            grad_ref.at[pl.ds(k * TAPS, TAPS)], grad_out.at[pl.ds(k * TAPS, TAPS)], sem.at[k]
        )
        for k in range(taps)
    ]
    copies.append(pltpu.make_async_copy(bias_ref, bias_out, sem.at[taps]))
    copies.append(pltpu.make_async_copy(head_ref, head_out, sem.at[taps + 1]))
    for copy in copies:
        copy.start()
    for copy in copies:
        copy.wait()


def per_device(sizes, clips, weight, bias, head):
    dp, tm, rows = sizes
    _, frames, _, cols, chans = clips.shape
    count = frames * cols
    plane = dp * rows
    share = chans // plane
    line, groups = split_line(tm, share // SUB)
    part = share // line
    taps = TAPS**2
    pair = 2 if rows % 2 == 0 else 1
    near = rows // pair
    if rows not in (1, 2, 4):
        raise ValueError("rows")
    sides = near - 1 + dp - 1
    turns = 2 * (near - 1) * (dp - 1)
    pad = pltpu.VMEM((frames + 2, 3, cols, chans), jnp.bfloat16)
    field = pltpu.VMEM((count, chans), jnp.float32)
    gathered = pltpu.VMEM((plane, frames, cols, chans), jnp.bfloat16)
    wide = WIDE if chans % WIDE == 0 else chans
    chunks = TAPS * (chans // wide)
    coded = pltpu.VMEM((chunks, line, taps + 1, part, wide), jnp.bfloat16)

    def dma(n):
        return pltpu.SemaphoreType.DMA((max(n, 1),))

    sems = []
    for send, recv in (
        (24, 24), (6, 6), (2 * dp * near, 2 * dp * near), (2 * dp * near, 2 * dp * near),
        (6, 6), (chunks, chunks),
        (chunks, chunks) if groups > 1 else (1, 1), (chunks, chunks * line),
        (chunks, chunks * line * sides), (chunks, chunks * line * max(1, turns // 2)),
        (chunks, chunks), (1, 1), (1, 1),
    ):
        sems += [dma(send), dma(recv)]
    vmem = pl.BlockSpec(memory_space=pltpu.VMEM)
    hbm = pl.BlockSpec(memory_space=pl.ANY)
    grad_weight, grad_bias, grad_head = pl.pallas_call(
        functools.partial(kernel, sizes, line),
        out_shape=(
            pltpu.VMEM((TAPS**3, chans, chans), jnp.float32),
            pltpu.VMEM((1, chans), jnp.float32),
            pltpu.VMEM((1, chans), jnp.float32),
        ),
        in_specs=[hbm, hbm, vmem, vmem],
        out_specs=(vmem, vmem, vmem),
        scratch_shapes=[
            pltpu.VMEM((TAPS**3, chans, chans), jnp.bfloat16),
            pltpu.VMEM((TAPS**3, chans, chans), jnp.bfloat16),
            pad, pad, pad,
            pltpu.VMEM((TAPS, count, chans), jnp.float32),
            field, field,
            gathered, gathered,
            pltpu.VMEM((2, frames, chans, cols), jnp.bfloat16),
            pltpu.VMEM((2, plane, frames + 2, share, cols), jnp.bfloat16),
            pltpu.VMEM((2, dp, rows + 2, frames + 2, TAPS * share, cols), jnp.bfloat16),
            pltpu.VMEM((TAPS, taps * share, chans), jnp.float32),
            pltpu.VMEM((chunks, line, taps, part, wide), jnp.float32),
            coded, coded,
            pltpu.VMEM((chunks, groups, taps + 1, part, wide), jnp.bfloat16),
            pltpu.VMEM((chunks, plane * line, taps + 1, part, wide), jnp.bfloat16),
            pltpu.VMEM((SUB, chans), jnp.float32),
            pltpu.VMEM((plane, SUB, chans), jnp.float32),
            pltpu.VMEM((tm, SUB, chans), jnp.float32),
            dma(3), *sems,
        ],
        compiler_params=pltpu.CompilerParams(
            collective_id=0, has_side_effects=True, vmem_limit_bytes=48 * 1024 * 1024
        ),
    )(
        pltpu.with_memory_space_constraint(clips.reshape(frames, cols, chans), pltpu.HBM),
        weight.reshape(TAPS**3, chans, chans),
        bias.reshape(1, chans),
        head.reshape(1, chans),
    )
    row = jax.ShapeDtypeStruct((1, chans), jnp.float32)
    grad_weight, grad_bias, grad_head = pl.pallas_call(
        put_out,
        out_shape=(jax.ShapeDtypeStruct((TAPS**3, chans, chans), jnp.float32), row, row),
        in_specs=[vmem, vmem, vmem],
        out_specs=(hbm, hbm, hbm),
        scratch_shapes=[pltpu.SemaphoreType.DMA((TAPS**2 + 2,))],
        compiler_params=pltpu.CompilerParams(vmem_limit_bytes=8 * 1024 * 1024),
    )(grad_weight, grad_bias, grad_head)
    grad_weight = grad_weight.reshape(TAPS, TAPS, TAPS, chans, chans)
    return grad_weight, grad_bias.reshape(chans), grad_head.reshape(chans)


def solution(mesh):
    sizes = tuple(mesh.shape[axis] for axis in ("dp", "tm", "rows"))
    return jax.shard_map(
        functools.partial(per_device, sizes),
        mesh=mesh,
        in_specs=(P("dp", "tm", "rows", None, None), P(), P(), P()),
        out_specs=(P(), P(), P()),
        check_vma=False,
    )
```

```python
import functools
import math

import jax
import jax.numpy as jnp
from jax import lax
from jax.experimental import pallas as pl
from jax.experimental.pallas import tpu as pltpu
from jax.sharding import PartitionSpec as P

penalty_weight = 0.01
MESH = pl.DeviceIdType.MESH
SUB = 8
TAPS = 3
SPAN = 120.0
LANES = 128
WIDE = 128


def split_line(tm, most):
    line = 1
    while tm % (2 * line) == 0 and 2 * line <= most:
        line *= 2
    return line, tm // line


def decode(block, taps):
    unit = block[taps].astype(jnp.float32) * (1.0 / (SPAN * math.log(2.0)))
    return jnp.log(block[:taps].astype(jnp.float32)) * unit[None]


def encode(value):
    top = (jnp.max(jnp.abs(value), axis=0) * 1.01 + 1e-30).astype(jnp.bfloat16)
    rate = SPAN / top.astype(jnp.float32)
    return jnp.exp2(value * rate[None]).astype(jnp.bfloat16), top


def kernel(
    sizes, line, clips_ref, weight_ref, bias_ref, head_ref,
    out_ref, bias_out, head_out,
    w_ref, wt_ref, clip_pad, score_pad, grad_pad, acc, slope_ref, curve_ref,
    clip_all, grad_all, turned, slices, shifts, first, total, code, land, more, full,
    small_mine, small_plane, small_line,
    local_sem, halo_send, halo_recv, hand_send, hand_recv, all_send, all_recv, pass_send, pass_recv,
    slice_send, slice_recv, part_send, part_recv, more_send, more_recv,
    line_send, line_recv, near_send, near_recv, turn_send, turn_recv, pair_send, pair_recv,
    sum_send, sum_recv, end_send, end_recv,
):
    dp, tm, rows = sizes
    frames, cols, chans = clips_ref.shape
    count = frames * cols
    plane = dp * rows
    share = chans // plane
    part = share // line
    taps = TAPS**2
    pair = 2 if rows % 2 == 0 else 1
    near = rows // pair
    me = {"dp": lax.axis_index("dp"), "tm": lax.axis_index("tm"), "rows": lax.axis_index("rows")}
    mine = me["dp"] * rows + me["rows"]

    def device(**moved):
        place = dict(me, **moved)
        return (place["dp"], place["tm"], place["rows"])

    def shift(axis, step):
        return lax.rem(me[axis] + step % dict(dp=dp, tm=tm, rows=rows)[axis], dict(dp=dp, tm=tm, rows=rows)[axis])

    def remote(src, dst, send, recv, target):
        return pltpu.make_async_remote_copy(
            src_ref=src, dst_ref=dst, send_sem=send, recv_sem=recv,
            device_id=target, device_id_type=MESH,
        )

    weight_copy = pltpu.make_async_copy(weight_ref, w_ref, local_sem.at[0])
    weight_copy.start()
    clip_copy = pltpu.make_async_copy(
        clips_ref, clip_pad.at[pl.ds(1, frames), 1], local_sem.at[1]
    )
    clip_copy.start()
    keep_copy = pltpu.make_async_copy(clips_ref, clip_all.at[mine], local_sem.at[2])
    keep_copy.start()

    steps = {(i, t % tm, s) for i in range(dp) for t in (-1, 0, 1) for s in range(rows)}
    steps |= {(0, t, 0) for t in range(tm)}
    steps = sorted(steps - {(0, 0, 0)})
    barrier = pltpu.get_barrier_semaphore()
    for i, t, s in steps:
        pl.semaphore_signal(
            barrier, inc=1, device_id=(shift("dp", i), shift("tm", t), shift("rows", s)),
            device_id_type=MESH,
        )
    def clear(pads):
        for axis, bound, fill in (
            ("rows", 0, lambda pad: pad.at[:, 0]), ("rows", rows - 1, lambda pad: pad.at[:, 2]),
            ("tm", 0, lambda pad: pad.at[0]), ("tm", tm - 1, lambda pad: pad.at[frames + 1]),
        ):
            @pl.when(me[axis] == bound)
            def _():
                for pad in pads:
                    at = fill(pad)
                    at[...] = jnp.zeros(at.shape, at.dtype)

    def clear_later():
        clear((score_pad, grad_pad))
        for which in range(2):
            for rim in (0, rows + 1):
                shifts[which, :, rim] = jnp.zeros(
                    shifts.shape[1:2] + shifts.shape[3:], shifts.dtype
                )
            for rim, bound in ((0, 0), (frames + 1, tm - 1)):
                @pl.when(me["tm"] == bound)
                def _():
                    slices[which, :, rim] = jnp.zeros((plane, share, cols), slices.dtype)

    clear((clip_pad,))
    pl.semaphore_wait(barrier, len(steps))

    moves = [(t, r) for t in (-1, 0, 1) for r in (-1, 0, 1) if (t, r) != (0, 0)]
    partner = me["rows"] + 1 - 2 * lax.rem(me["rows"], 2) if pair == 2 else me["rows"]
    mirror = rows - 1 - me["rows"]
    toward = partner - me["rows"]

    def inside(t, r):
        ok = None
        for axis, step, size in (("tm", t, tm), ("rows", r, rows)):
            if step:
                cond = me[axis] > 0 if step < 0 else me[axis] < size - 1
                ok = cond if ok is None else jnp.logical_and(ok, cond)
        return ok

    def leaves(t, r, sender):
        ok = inside(t, r) if sender else inside(-t, -r)
        if pair == 1:
            return ok
        row = me["rows"] if sender else me["rows"] - r
        return jnp.logical_and(ok, lax.rem(row, 2) == (0 if r < 0 else 1))

    def halo_copy(which, pad, source, t, r):
        slot = which * len(moves) + moves.index((t, r))
        if t == 0:
            here, there = pl.ds(0, frames), pl.ds(1, frames)
        elif t > 0:
            here, there = pl.ds(frames - 1, 1), pl.ds(0, 1)
        else:
            here, there = pl.ds(0, 1), pl.ds(frames + 1, 1)
        return remote(
            source.at[here], pad.at[there, 1 - r], halo_send.at[slot], halo_recv.at[slot],
            device(tm=me["tm"] + t, rows=me["rows"] + r),
        )

    def hand_copy(which, pad, t):
        at = 2 * which + (t > 0)
        edge = 0 if t > 0 else frames + 1
        return remote(
            pad.at[edge, 1], pad.at[edge, 1 - toward], hand_send.at[at], hand_recv.at[at],
            device(rows=partner),
        )

    def depth_start(which, pad, source):
        for t in (-1, 1):
            @pl.when(inside(t, 0))
            def _():
                halo_copy(which, pad, source, t, 0).start()

    def side_start(which, pad, source):
        for r in (-1, 1):
            @pl.when(inside(0, r))
            def _():
                halo_copy(which, pad, source, 0, r).start()

    def corner_start(which, pad, source):
        for t in (-1, 1):
            for r in (-1, 1):
                @pl.when(leaves(t, r, True))
                def _():
                    halo_copy(which, pad, source, t, r).start()

    def side_sent(which, pad, source):
        for r in (-1, 1):
            @pl.when(inside(0, r))
            def _():
                halo_copy(which, pad, source, 0, r).wait_send()

    def side_wait(which, pad, source, close):
        for r in (-1, 1):
            here = leaves(0, r, False)
            if close:
                here = jnp.logical_and(inside(0, -r), jnp.logical_not(here))

            @pl.when(here)
            def _():
                halo_copy(which, pad, source, 0, r).wait_recv()

    def depth_wait(which, pad, source):
        for t in (-1, 1):
            @pl.when(inside(-t, 0))
            def _():
                halo_copy(which, pad, source, t, 0).wait_recv()
                if pair == 2:
                    hand_copy(which, pad, t).start()
        for t in (-1, 1):
            @pl.when(inside(t, 0))
            def _():
                halo_copy(which, pad, source, t, 0).wait_send()

    def corner_wait(which, pad, source):
        for t in (-1, 1):
            for r in (-1, 1):
                @pl.when(leaves(t, r, True))
                def _():
                    halo_copy(which, pad, source, t, r).wait_send()

                @pl.when(leaves(t, r, False))
                def _():
                    halo_copy(which, pad, source, t, r).wait_recv()

    def hand_wait(which, pad):
        for t in (-1, 1):
            if pair == 2:
                @pl.when(inside(-t, 0))
                def _():
                    hand_copy(which, pad, t).wait()

    column = lax.rem(lax.broadcasted_iota(jnp.int32, (count, chans), 0), cols)

    def earlier(value):
        return jnp.where(column == 0, 0.0, pltpu.roll(value, 1, 0))

    def later(value):
        return jnp.where(column == cols - 1, 0.0, pltpu.roll(value, count - 1, 0))

    def conv(which, pad, source, kernel_ref, idle, sent, side, before, after, between):
        def put(shift_f, start, many, places, new=False):
            if not many or not places:
                return
            left = jnp.concatenate(
                [
                    pad[pl.ds(start + shift_f, many), b].reshape(many * cols, chans)
                    for b in places
                ],
                axis=1,
            )
            at = pl.ds(start * cols, many * cols)
            for d in range(TAPS):
                taps = [kernel_ref[(shift_f * TAPS + b) * TAPS + d] for b in places]
                value = jnp.dot(
                    left, jnp.concatenate(taps, axis=0), preferred_element_type=jnp.float32
                )
                acc[d, at] = value if new else acc[d, at] + value

        def inner_frames(places, new):
            put(1, 0, frames, places, new)
            put(0, 1, frames - 1, places)
            put(2, 0, frames - 1, places)

        def outer_frames(places):
            put(0, 0, 1, places)
            put(2, frames - 1, 1, places)

        close, far = ((1 + toward,), (1 - toward,)) if pair == 2 else ((), (0, 2))
        inner_frames((1,), True)
        corner_start(which, pad, source)
        idle()
        side(which, pad, source, True)
        inner_frames(close, False)
        before()
        depth_wait(which, pad, source)
        outer_frames((1,))
        hand_wait(which, pad)
        outer_frames(close)
        after()
        side(which, pad, source, False)
        between()
        inner_frames(far, False)
        corner_wait(which, pad, source)
        outer_frames(far)
        sent()
        return earlier(acc[0]) + acc[1] + later(acc[2])

    others = range(1, dp)
    across = [(0, 0)] + [(i, 0) for i in others]
    if near == 2:
        across = [(0, 0), (0, 1)] + [(i, 0) for i in others] + [(i, 1) for i in others]

    edge = jnp.logical_and(me["rows"] > 0, me["rows"] < rows - 1)

    def spot(i, m):
        return shift("dp", -i) * rows + (mirror if m else me["rows"])

    def all_copy(which, buf, i, m):
        at = which * len(across) + across.index((i, m))
        if i == 0:
            block, there = buf.at[mine], device(rows=mirror)
        else:
            block, there = buf.at[spot(0, m)], device(dp=shift("dp", i))
        return remote(block, block, all_send.at[at], all_recv.at[at], there)

    def pass_copy(which, buf, i, m):
        at = which * len(across) + across.index((i, m))
        block = buf.at[spot(i, m)]
        return remote(block, block, pass_send.at[at], pass_recv.at[at], device(rows=partner))

    def all_start(which, buf):
        if pair == 2:
            pass_copy(which, buf, 0, 0).start()
        if near == 2:
            @pl.when(edge)
            def _():
                all_copy(which, buf, 0, 1).start()

    def all_down(which, buf):
        for i in others:
            all_copy(which, buf, i, 0).start()

    def all_side(buf):
        def side(which, pad, source, close):
            at = which // 2
            if pair == 2 and close:
                pass_copy(at, buf, 0, 0).wait_recv()
                pad[pl.ds(1, frames), 1 + toward] = buf[me["dp"] * rows + partner]
            if near == 2 and not close:
                @pl.when(edge)
                def _():
                    all_copy(at, buf, 0, 1).wait_recv()
                    pad[pl.ds(1, frames), 1 - toward] = buf[me["dp"] * rows + mirror]

        return side

    def all_sent(which, buf):
        if near == 2:
            @pl.when(edge)
            def _():
                all_copy(which, buf, 0, 1).wait_send()

    def far_copy(which, buf, i):
        at = which * len(across) + across.index((i, 1))
        block = buf.at[mine]
        return remote(
            block, block, all_send.at[at], all_recv.at[at],
            device(dp=shift("dp", i), rows=mirror),
        )

    def all_between(which, buf):
        if near == 2:
            @pl.when(edge)
            def _():
                for i in others:
                    all_copy(which, buf, i, 1).start()
                pass_copy(which, buf, 0, 1).start()

    def all_outer(which, buf):
        if near == 2:
            @pl.when(jnp.logical_not(edge))
            def _():
                all_copy(which, buf, 0, 1).start()
                for i in others:
                    far_copy(which, buf, i).start()

    def all_relay(which, buf):
        if near == 2:
            @pl.when(jnp.logical_not(edge))
            def _():
                all_copy(which, buf, 0, 1).wait_recv()
                pass_copy(which, buf, 0, 1).start()

    def all_near(which, buf):
        if near == 2:
            pass_copy(which, buf, 0, 1).wait_recv()

    def all_far(which, buf, m):
        if m and near != 2:
            return
        for i in others:
            all_copy(which, buf, i, m).wait_recv()
            if pair == 2:
                pass_copy(which, buf, i, m).start()

    def all_end(which, buf):
        for i, m in across:
            if (i, m) == (0, 1):
                @pl.when(jnp.logical_not(edge))
                def _():
                    all_copy(which, buf, i, m).wait_send()
            elif i:
                all_copy(which, buf, i, m).wait_send()
            if pair == 2:
                pass_copy(which, buf, i, m).wait_send()
                if i:
                    pass_copy(which, buf, i, m).wait_recv()

    def slice_copy(which, t, i, s):
        at = which * 3 + t + 1
        y, r = shift("dp", i), shift("rows", s)
        rest = pl.ds(pl.multiple_of((y * rows + r) * share, share), share)
        if t == 0:
            src, dst = turned.at[which, :, rest], slices.at[which, mine, pl.ds(1, frames)]
        elif t > 0:
            src, dst = turned.at[which, frames - 1, rest], slices.at[which, mine, 0]
        else:
            src, dst = turned.at[which, 0, rest], slices.at[which, mine, frames + 1]
        return remote(
            src, dst, slice_send.at[at], slice_recv.at[at],
            device(dp=y, rows=r, tm=me["tm"] + t),
        )

    pieces = [(i, s) for i in range(dp) for s in range(rows)]

    def slice_turn(which, value):
        for f in range(frames):
            turned[which, f] = value[f].T

    def slice_start(which):
        for t in (1, -1):
            @pl.when(inside(t, 0))
            def _():
                for i, s in pieces:
                    slice_copy(which, t, i, s).start()
        for i, s in pieces[1:]:
            slice_copy(which, 0, i, s).start()
        own = pl.ds(pl.multiple_of(mine * share, share), share)
        for f in range(frames):
            slices[which, mine, f + 1] = turned[which, f, own]

    lane = lax.broadcasted_iota(jnp.int32, (share, cols), 1)

    def slice_end(which):
        def whole(t):
            at = which * 3 + t + 1
            block = slices.at[which, :, 0] if t else slices.at[
                which, pl.ds(0, plane - 1), pl.ds(1, frames)
            ]
            return remote(block, block, slice_send.at[at], slice_recv.at[at], device())

        for t in (1, -1):
            @pl.when(inside(t, 0))
            def _():
                whole(t).wait_send()

            @pl.when(inside(-t, 0))
            def _():
                whole(t).wait_recv()
        whole(0).wait()
        for j in range(plane):
            for f in range(frames + 2):
                value = slices[which, j, f].astype(jnp.float32)
                after = jnp.where(lane == cols - 1, 0.0, pltpu.roll(value, cols - 1, 1))
                before = jnp.where(lane == 0, 0.0, pltpu.roll(value, 1, 1))
                shifts[which, j // rows, j % rows + 1, f] = jnp.concatenate(
                    [after, value, before], axis=0
                ).astype(jnp.bfloat16)

    def correlate(which, buf, a, clips):
        left = jnp.concatenate(
            [
                jnp.concatenate(
                    [
                        shifts[which, y, r + 2 - b, f + 2 - a]
                        for y in clips for r in range(rows) for f in range(frames)
                    ],
                    axis=1,
                )
                for b in range(TAPS)
            ],
            axis=0,
        )
        right = jnp.concatenate(
            [buf[pl.ds(y * rows, rows)].reshape(rows * count, chans) for y in clips], axis=0
        )
        return jnp.dot(left, right, preferred_element_type=jnp.float32)

    def turn_weight():
        def one(k, carry):
            wt_ref[TAPS**3 - 1 - k] = w_ref[k].T
            return carry

        lax.fori_loop(0, TAPS**3, one, 0, unroll=3)
        clear_later()

    depth_start(0, clip_pad, clips_ref)
    clip_copy.wait()
    keep_copy.wait()
    all_start(0, clip_all)
    all_down(0, clip_all)
    weight_copy.wait()
    pre = bias_ref[...] + conv(
        0, clip_pad, clips_ref, w_ref, turn_weight, lambda: all_sent(0, clip_all),
        all_side(clip_all), lambda: all_outer(0, clip_all), lambda: None,
        lambda: all_between(0, clip_all),
    )
    sig = jax.nn.sigmoid(pre)
    slope = sig * (1.0 + pre * (1.0 - sig))
    slope_ref[...] = slope
    curve_ref[...] = sig * (1.0 - sig) * (2.0 + pre * (1.0 - 2.0 * sig))
    score = (head_ref[...] * slope).astype(jnp.bfloat16)
    score_pad[pl.ds(1, frames), 1] = score.reshape(frames, cols, chans)
    score_own = score_pad.at[pl.ds(1, frames), 1]
    depth_start(1, score_pad, score_own)
    side_start(1, score_pad, score_own)
    all_relay(0, clip_all)
    all_far(0, clip_all, 0)

    input_grad = conv(
        1, score_pad, score_own, wt_ref, lambda: None,
        lambda: side_sent(1, score_pad, score_own), side_wait, lambda: None,
        lambda: slice_turn(0, score_pad[pl.ds(1, frames), 1]),
        lambda: slice_start(0),
    ).astype(jnp.bfloat16).reshape(frames, cols, chans)
    grad_pad[pl.ds(1, frames), 1] = input_grad
    grad_all[mine] = input_grad
    grad_own = grad_pad.at[pl.ds(1, frames), 1]
    depth_start(2, grad_pad, grad_own)
    all_start(1, grad_all)
    all_down(1, grad_all)
    all_far(0, clip_all, 1)

    back = penalty_weight * conv(
        2, grad_pad, grad_own, w_ref, lambda: None,
        lambda: (all_relay(1, grad_all), all_sent(1, grad_all)),
        all_side(grad_all), lambda: all_outer(1, grad_all), lambda: None,
        lambda: all_between(1, grad_all),
    )
    pre_grad = back * head_ref[...] * curve_ref[...]
    slice_turn(
        1, pre_grad.astype(jnp.bfloat16).reshape(frames, cols, chans)
    )
    slice_start(1)
    small_mine[...] = jnp.zeros_like(small_mine)
    small_mine[pl.ds(0, 1)] = jnp.sum(pre_grad, axis=0, keepdims=True)
    small_mine[pl.ds(1, 1)] = jnp.sum(back * slope_ref[...], axis=0, keepdims=True)

    def sum_copy(i, s):
        return remote(
            small_mine, small_plane.at[mine], sum_send.at[0], sum_recv.at[0],
            device(dp=shift("dp", i), rows=shift("rows", s)),
        )

    small_plane[mine] = small_mine[...]
    for i, s in pieces[1:]:
        sum_copy(i, s).start()

    slice_end(0)
    all_far(1, grad_all, 0)
    all_near(0, clip_all)
    all_end(0, clip_all)
    all_near(1, grad_all)
    for a in range(TAPS):
        first[a] = correlate(0, grad_all, a, [me["dp"]])
    all_far(1, grad_all, 1)
    slice_end(1)
    for a in range(TAPS):
        first[a] = penalty_weight * first[a] + correlate(1, clip_all, a, range(dp))
    all_end(1, grad_all)
    inner, outer = lax.rem(me["tm"], line), me["tm"] // line
    wide = full.shape[-1]
    chunks = [(a, low) for a in range(TAPS) for low in range(chans // wide)]

    def along(step):
        return lax.rem(inner + step, line)

    def part_copy(c, step):
        return remote(
            code.at[c, along(step)], land.at[c, inner], part_send.at[c], part_recv.at[c],
            device(tm=outer * line + along(step)),
        )

    def part_all(c):
        block = land.at[c, pl.ds(0, line - 1)]
        return remote(block, block, part_send.at[c], part_recv.at[c], device())

    def product(a):
        both = first[a]
        if dp > 1:
            both = both + penalty_weight * correlate(
                0, grad_all, a, [shift("dp", i) for i in others]
            )
        both = both.reshape(taps, share, chans)
        for k in range(chans // wide):
            for t in range(line):
                total[a * (chans // wide) + k, t] = both[
                    :, t * part : (t + 1) * part, k * wide : (k + 1) * wide
                ]

    def scatter(c):
        for step in range(line - 1, 0, -1):
            value, top = encode(total[c, along(step)])
            code[c, along(step), pl.ds(0, taps)] = value
            code[c, along(step), taps] = top
        if c >= 1 and line > 1:
            part_all(c - 1).wait_send()
        for step in range(line - 1, 0, -1):
            part_copy(c, step).start()

    groups = tm // line

    def more_copy(c, step):
        spot = lax.rem(outer + step, groups)
        return remote(
            more.at[c, outer], more.at[c, outer], more_send.at[c], more_recv.at[c],
            device(tm=spot * line + inner),
        )

    upper = inner // 2
    ranks = [inner, inner + 1 - 2 * lax.rem(inner, 2), 2 - upper, 3 - 3 * upper][:line]
    middle = lax.rem(inner + upper, 2) == 1

    def line_copy(c, rank, to):
        here = full.at[c, mine * line + ranks[rank]]
        return remote(
            here, here, line_send.at[c], line_recv.at[c * line + ranks[rank]],
            device(tm=outer * line + to),
        )

    def collect(c):
        value = total[c, inner]
        if line > 1:
            part_all(c).wait_recv()
            if c >= len(chunks) - 1:
                part_all(c).wait_send()
        for step in range(1, line):
            value = value + decode(land[c, along(step)], taps)
        if groups > 1:
            value, top = encode(value)
            more[c, outer, pl.ds(0, taps)] = value
            more[c, outer, taps] = top
            for step in range(1, groups):
                more_copy(c, step).start()
            block = more.at[c, pl.ds(0, groups - 1)]
            remote(block, block, more_send.at[c], more_recv.at[c], device()).wait()
            value = decode(more[c, 0], taps)
            for k in range(1, groups):
                value = value + decode(more[c, k], taps)
        value, top = encode(value)
        full[c, mine * line + inner, pl.ds(0, taps)] = value
        full[c, mine * line + inner, taps] = top
        for rank in range(min(line - 1, 2), 0, -1):
            line_copy(c, 0, ranks[rank]).start()
        share_out(c, 0)

    def share_out(c, rank):
        for side in sides:
            near_copy(c, rank, side).start()
        if pair == 2:
            pair_copy(c, rank, 0).start()

    def take(c, rank):
        if rank > 1:
            @pl.when(jnp.logical_not(middle))
            def _():
                line_copy(c, rank, inner).wait_recv()
        else:
            line_copy(c, rank, inner).wait_recv()
        share_out(c, rank)

    def onward(c):
        if line == 4:
            @pl.when(middle)
            def _():
                for rank in (2, 3):
                    line_copy(c, rank, inner).wait_recv()
                    line_copy(c, rank, ranks[1]).start()

    sides = [("rows", s) for s in range(1, near)] + [("dp", i) for i in range(1, dp)]

    def go(side):
        axis, step = side
        return {axis: shift(axis, step * (pair if axis == "rows" else 1))}

    def come(side):
        axis, step = side
        return {axis: shift(axis, -step * (pair if axis == "rows" else 1))}

    def number(place):
        place = dict(me, **place)
        return place["dp"] * rows + place["rows"]

    turns = [(one, two) for one in sides for two in sides if one[0] != two[0]]
    hops = [()] + [(side,) for side in sides] + turns

    def block_at(c, rank, hop):
        place = {}
        for side in hop:
            place.update(come(side))
        return full.at[c, number(place) * line + ranks[rank]]

    def turned_by(rank):
        return [turn for turn in turns if turn[0][0] == ("dp" if rank % 2 else "rows")]

    per_turn = max(1, len(turns) // 2)

    def near_copy(c, rank, side):
        at = (c * line + rank) * len(sides) + sides.index(side)
        block = block_at(c, rank, ())
        return remote(block, block, near_send.at[c], near_recv.at[at], device(**go(side)))

    def turn_copy(c, rank, turn):
        at = (c * line + rank) * per_turn + turned_by(rank).index(turn)
        block = block_at(c, rank, turn[:1])
        return remote(block, block, turn_send.at[c], turn_recv.at[at], device(**go(turn[1])))

    def pair_copy(c, rank, k):
        block = block_at(c, rank, hops[k])
        return remote(block, block, pair_send.at[c], pair_recv.at[c], device(rows=partner))

    def relay(c, rank):
        for k, side in enumerate(sides):
            near_copy(c, rank, side).wait_recv()
            for turn in turned_by(rank):
                if turn[0] == side:
                    turn_copy(c, rank, turn).start()
            if pair == 2:
                pair_copy(c, rank, 1 + k).start()

    def handover(c, rank):
        for turn in turned_by(rank):
            turn_copy(c, rank, turn).wait_recv()
            if pair == 2:
                pair_copy(c, rank, hops.index(turn)).start()

    def finish(c):
        a, low = chunks[c]
        ended = [(near_send, line * len(sides)), (turn_send, sum(len(turned_by(k)) for k in range(line)))]
        for sem, n in ended + [(line_send, min(line - 1, 2))]:
            if n:
                block = full.at[c, pl.ds(0, n)]
                remote(block, block, sem.at[c], sem.at[c], device()).wait_send()
        if line == 4:
            @pl.when(middle)
            def _():
                block = full.at[c, pl.ds(0, 2)]
                remote(block, block, line_send.at[c], line_send.at[c], device()).wait_send()
        if pair == 2:
            block = full.at[c, pl.ds(0, plane * line // 2)]
            remote(block, block, pair_send.at[c], pair_recv.at[c], device()).wait()
        per = LANES // part

        def tap(k, carry):
            for high in range(chans // LANES):
                for left in range(0, wide, LANES):
                    pile = []
                    for n in range(high * per, (high + 1) * per):
                        block = full.at[c, n]
                        unit = block[taps, :, left : left + LANES].astype(jnp.float32)
                        value = jnp.log(block[k, :, left : left + LANES].astype(jnp.float32))
                        pile.append(value * (unit * (1.0 / (SPAN * math.log(2.0)))))
                    out_ref[
                        a * taps + k, low * wide + left : low * wide + left + LANES,
                        high * LANES : (high + 1) * LANES,
                    ] = jnp.concatenate(pile, axis=0).T
            return carry

        lax.fori_loop(0, taps, tap, 0, unroll=True)

    def end_copy(step):
        return remote(
            small_mine, small_line.at[me["tm"]], end_send.at[0], end_recv.at[0],
            device(tm=shift("tm", step)),
        )

    def small_middle():
        block = small_plane.at[pl.ds(0, plane - 1)]
        if plane > 1:
            remote(block, block, sum_send.at[0], sum_recv.at[0], device()).wait()
        small_mine[...] = jnp.sum(small_plane[...], axis=0)
        small_line[me["tm"]] = small_mine[...]
        for step in range(1, tm):
            end_copy(step).start()

    def small_end():
        block = small_line.at[pl.ds(0, tm - 1)]
        if tm > 1:
            remote(block, block, end_send.at[0], end_recv.at[0], device()).wait()
        value = jnp.sum(small_line[...], axis=0)
        bias_out[...] = value[0:1]
        head_out[...] = value[1:2]

    pace = 2.65 * wide / LANES
    order = [(4.0, small_middle, ()), (16.0, small_end, ()), (-9.0, product, (0,))]
    order += [(got_a, product, (a,)) for a, got_a in ((1, 0.1), (2, 2.0))]
    for c in range(len(chunks)):
        got = 4.9 + pace * c
        order += [
            (got - 5.2, scatter, (c,)), (got, collect, (c,)), (got + 2.8, onward, (c,)),
            (got + 23.0, finish, (c,)),
        ]
        for rank in range(line):
            if rank:
                order.append((got + (0, 2.9, 5.4, 5.5)[rank], take, (c, rank)))
            order += [
                (got + (7.0, 10.0, 12.2, 12.3)[rank], relay, (c, rank)),
                (got + (13.2, 16.0, 19.0, 19.1)[rank], handover, (c, rank)),
            ]
    for _, stage, what in sorted(order, key=lambda entry: entry[0]):
        stage(*what)


def put_out(grad_ref, bias_ref, head_ref, grad_out, bias_out, head_out, sem):
    taps = TAPS**2
    copies = [
        pltpu.make_async_copy(
            grad_ref.at[pl.ds(k * taps, taps)], grad_out.at[pl.ds(k * taps, taps)], sem.at[k]
        )
        for k in range(TAPS)
    ]
    copies.append(pltpu.make_async_copy(bias_ref, bias_out, sem.at[TAPS]))
    copies.append(pltpu.make_async_copy(head_ref, head_out, sem.at[TAPS + 1]))
    for copy in copies:
        copy.start()
    for copy in copies:
        copy.wait()


def per_device(sizes, clips, weight, bias, head):
    dp, tm, rows = sizes
    _, frames, _, cols, chans = clips.shape
    count = frames * cols
    plane = dp * rows
    share = chans // plane
    line, groups = split_line(tm, share // SUB)
    part = share // line
    taps = TAPS**2
    pair = 2 if rows % 2 == 0 else 1
    near = rows // pair
    if rows not in (1, 2, 4):
        raise ValueError("rows")
    sides = near - 1 + dp - 1
    turns = 2 * (near - 1) * (dp - 1)
    pad = pltpu.VMEM((frames + 2, 3, cols, chans), jnp.bfloat16)
    field = pltpu.VMEM((count, chans), jnp.float32)
    gathered = pltpu.VMEM((plane, frames, cols, chans), jnp.bfloat16)
    wide = WIDE if chans % WIDE == 0 else chans
    chunks = TAPS * (chans // wide)
    coded = pltpu.VMEM((chunks, line, taps + 1, part, wide), jnp.bfloat16)

    def dma(n):
        return pltpu.SemaphoreType.DMA((max(n, 1),))

    sems = []
    for send, recv in (
        (24, 24), (6, 6), (2 * dp * near, 2 * dp * near), (2 * dp * near, 2 * dp * near),
        (6, 6), (chunks, chunks),
        (chunks, chunks) if groups > 1 else (1, 1), (chunks, chunks * line),
        (chunks, chunks * line * sides), (chunks, chunks * line * max(1, turns // 2)),
        (chunks, chunks), (1, 1), (1, 1),
    ):
        sems += [dma(send), dma(recv)]
    vmem = pl.BlockSpec(memory_space=pltpu.VMEM)
    hbm = pl.BlockSpec(memory_space=pl.ANY)
    grad_weight, grad_bias, grad_head = pl.pallas_call(
        functools.partial(kernel, sizes, line),
        out_shape=(
            pltpu.VMEM((TAPS**3, chans, chans), jnp.float32),
            pltpu.VMEM((1, chans), jnp.float32),
            pltpu.VMEM((1, chans), jnp.float32),
        ),
        in_specs=[hbm, hbm, vmem, vmem],
        out_specs=(vmem, vmem, vmem),
        scratch_shapes=[
            pltpu.VMEM((TAPS**3, chans, chans), jnp.bfloat16),
            pltpu.VMEM((TAPS**3, chans, chans), jnp.bfloat16),
            pad, pad, pad,
            pltpu.VMEM((TAPS, count, chans), jnp.float32),
            field, field,
            gathered, gathered,
            pltpu.VMEM((2, frames, chans, cols), jnp.bfloat16),
            pltpu.VMEM((2, plane, frames + 2, share, cols), jnp.bfloat16),
            pltpu.VMEM((2, dp, rows + 2, frames + 2, TAPS * share, cols), jnp.bfloat16),
            pltpu.VMEM((TAPS, taps * share, chans), jnp.float32),
            pltpu.VMEM((chunks, line, taps, part, wide), jnp.float32),
            coded, coded,
            pltpu.VMEM((chunks, groups, taps + 1, part, wide), jnp.bfloat16),
            pltpu.VMEM((chunks, plane * line, taps + 1, part, wide), jnp.bfloat16),
            pltpu.VMEM((SUB, chans), jnp.float32),
            pltpu.VMEM((plane, SUB, chans), jnp.float32),
            pltpu.VMEM((tm, SUB, chans), jnp.float32),
            dma(3), *sems,
        ],
        compiler_params=pltpu.CompilerParams(
            collective_id=0, has_side_effects=True, vmem_limit_bytes=48 * 1024 * 1024
        ),
    )(
        pltpu.with_memory_space_constraint(clips.reshape(frames, cols, chans), pltpu.HBM),
        weight.reshape(TAPS**3, chans, chans),
        bias.reshape(1, chans),
        head.reshape(1, chans),
    )
    row = jax.ShapeDtypeStruct((1, chans), jnp.float32)
    grad_weight, grad_bias, grad_head = pl.pallas_call(
        put_out,
        out_shape=(jax.ShapeDtypeStruct((TAPS**3, chans, chans), jnp.float32), row, row),
        in_specs=[vmem, vmem, vmem],
        out_specs=(hbm, hbm, hbm),
        scratch_shapes=[pltpu.SemaphoreType.DMA((TAPS + 2,))],
        compiler_params=pltpu.CompilerParams(vmem_limit_bytes=8 * 1024 * 1024),
    )(grad_weight, grad_bias, grad_head)
    grad_weight = grad_weight.reshape(TAPS, TAPS, TAPS, chans, chans)
    return grad_weight, grad_bias.reshape(chans), grad_head.reshape(chans)


def solution(mesh):
    sizes = tuple(mesh.shape[axis] for axis in ("dp", "tm", "rows"))
    return jax.shard_map(
        functools.partial(per_device, sizes),
        mesh=mesh,
        in_specs=(P("dp", "tm", "rows", None, None), P(), P(), P()),
        out_specs=(P(), P(), P()),
        check_vma=False,
    )
```
